32 devices in a mesh: grp: 2 (over x), seq: 16 (over z, y, core).
Axes of the slice: x: 2, y: 2, z: 4, core: 2. Of those that a mesh axis runs over, the one named last changes fastest.
Arguments:
- cont_query: bfloat16 [64, 32, 2560], P(('grp', 'seq')), parts along dimension 0, may hold values from -180 to 180
- cont_key: bfloat16 [64, 32, 512], P(('grp', 'seq')), parts along dimension 0, may hold values from -6 to 6
- cont_value: bfloat16 [64, 32, 512], P(('grp', 'seq')), parts along dimension 0, may hold values from -6 to 6
- prefix_key: bfloat16 [4, 2048, 512], P('grp', 'seq'), parts along dimension 0, may hold values from -7 to 7
- prefix_value: bfloat16 [4, 2048, 512], P('grp', 'seq'), parts along dimension 0, may hold values from -6 to 6
- out_weight: bfloat16 [2560, 2560], P(None, 'seq'), may hold values from -0.125 to 0.125
- norm_gain: float32 [2560], replicated, may hold values from 0.5 to 1.5
- lm_head: bfloat16 [2560, 76032], P(None, 'seq'), may hold values from -18 to 18
- target_ids: int32 [64, 32], P(('grp', 'seq')), parts along dimension 0, may hold values from 0 to 76031
- cont_len: int32 [64], P(('grp', 'seq')), parts along dimension 0, may hold values from 8 to 32
- prompt_len: int32 [4], P('grp'), parts along dimension 0, may hold values from 1024 to 2048
- group_of: int32 [64], P('grp'), parts along dimension 0, may hold values from 0 to 1, as said below
- rewards: float32 [64], P(('grp', 'seq')), parts along dimension 0, may hold values from -13 to 13
Outputs:
- token_logprob: float32 [64, 32], P(('grp', 'seq')), parts along dimension 0
- advantage: float32 [64], P(('grp', 'seq')), parts along dimension 0
- objective: float32 [64], P(('grp', 'seq')), parts along dimension 0
The draws below stay inside these ranges and needn't reach their ends.
There are 2 independent parts, one for each index of `grp`. The reference program is written for one: setup_inputs(seed, part) draws one part's arguments, and reference() takes and returns one part's arrays. A program takes and returns all parts, laid end to end along the dimension named above; an argument that names none is the same for every part. Nothing has to cross between parts.
Inputs may be any that keep to these rules, and one draw needn't show every extreme that they name: `group_of`: each of the 2 prompts is named by exactly 16 continuations.
All inputs are finite; a program needn't handle non-finite values.
Results may differ from the reference program's by a relative error of at most 0.0026.
Values may be sent and summed in bfloat16 or wider, within the bound.
A program may use at most 128 MiB of HBM per device.

```python
import math
import jax
import jax.numpy as jnp
import numpy as np
from jax import lax

D = 2560
QH = 20
KVH = 4
HD = 128
VOCAB = 76032
GROUP = 16
CLEN = 32
PROMPT = 2048
CONTS = 32
PROMPTS = 2
N_SEQ = 16


def draw_groups(key):
    shuffled = jax.random.permutation(jax.random.fold_in(key, 11), CONTS)
    return (shuffled // GROUP).astype(jnp.int32)


def draw_group_of(key, part):
    return draw_groups(key)


def draw_prefix_key(key, part):
    drawn = jnp.clip(jax.random.normal(jax.random.fold_in(key, 13), (PROMPTS, PROMPT, KVH * HD), jnp.float32), -6.0, 6.0)
    return drawn.astype(jnp.bfloat16)


def draw_cont_query(key, part):
    drawn = jnp.clip(jax.random.normal(jax.random.fold_in(key, 14), (CONTS, CLEN, QH * HD), jnp.float32), -6.0, 6.0)
    return drawn.astype(jnp.bfloat16)


def draw_lm_head(key, part):
    drawn = jnp.clip(jax.random.normal(jax.random.fold_in(key, 19), (D, VOCAB), jnp.float32), -6.0, 6.0)
    column_scale = jnp.full((1, VOCAB), 3.0 / math.sqrt(D), jnp.float32)
    return (drawn * column_scale).astype(jnp.bfloat16)


def draw_rewards(key, part):
    groups = draw_groups(key)
    spread = jnp.exp(jax.random.uniform(jax.random.fold_in(key, 16), (PROMPTS,), jnp.float32, math.log(0.05), math.log(2.0)))
    offset = jax.random.uniform(jax.random.fold_in(key, 17), (PROMPTS,), jnp.float32, -1.0, 1.0)
    jitter = jnp.clip(jax.random.normal(jax.random.fold_in(key, 18), (CONTS,), jnp.float32), -6.0, 6.0)
    return offset[groups] + spread[groups] * jitter


def place_ends(array, own_key, smallest, largest):
    shape = array.shape
    index_at = [jax.random.randint(jax.random.fold_in(own_key, axis), (), 0, shape[axis]) for axis in range(len(shape))]
    array = array.at[tuple(index_at)].set(smallest)
    longest = shape.index(max(shape))
    index_at[longest] = (index_at[longest] + 1) % shape[longest]
    return array.at[tuple(index_at)].set(largest)


def level_of(stream_key, dims, pieces, least, largest):
    factor_of = 1.0
    for axis_at, blocks in pieces:
        draws = jax.random.uniform(jax.random.fold_in(jax.random.fold_in(stream_key, 6), axis_at), (blocks,), jnp.float32, least / len(pieces), largest / len(pieces))
        factor_of = factor_of * jnp.repeat(jnp.exp(draws), dims[axis_at] // blocks).reshape((-1,) + (1,) * (len(dims) - 1 - axis_at))
    return factor_of


def skewed_wide(stream_key, dims, number_of, lean):
    loads = [min(1 << octave, number_of + 1 - (1 << octave)) * (1 << 20) // math.isqrt((1 << octave) ** lean) + 1 for octave in range((number_of + 1).bit_length()) if 1 << octave <= number_of]
    width = 1 + sum(loads) // (1 << 30)
    listing = np.cumsum(np.array([max(1, weight // width) for weight in loads]))
    ticket = jax.random.randint(jax.random.fold_in(stream_key, 1), dims, 0, int(listing[len(loads) - 1]))
    start = jnp.left_shift(1, jnp.searchsorted(jnp.asarray(listing, jnp.int32), ticket, side="right").astype(jnp.int32))
    grade = start - 1 + jax.random.randint(jax.random.fold_in(stream_key, 4), dims, 0, 1 << 30) % jnp.minimum(start, number_of + 1 - start)
    return jax.random.permutation(jax.random.fold_in(stream_key, 2), number_of)[grade].astype(jnp.int32)


def bell_draw(own_key, shape, scale, bound, shards=(), held_as=jnp.bfloat16):
    values = scale * jax.random.normal(own_key, shape, jnp.float32)
    if shards:
        values = values * level_of(own_key, shape, shards, -0.22, 0.18)
    return jnp.clip(values, -bound, bound).astype(held_as)


def setup_inputs(seed: int = 0, part: int = 0) -> dict:
    key_list = jax.random.split(jax.random.key(seed), 14)
    part_keys = jax.random.split(jax.random.fold_in(key_list[13], part), 14)
    return {
        "cont_query": draw_cont_query(jax.random.fold_in(jax.random.fold_in(key_list[13], part), 71), part),
        "cont_key": bell_draw(part_keys[1], (CONTS, CLEN, KVH * HD), 1.0, 6.0, ((0, 16),)),
        "cont_value": bell_draw(part_keys[2], (CONTS, CLEN, KVH * HD), 1.0, 6.0, ((0, 16),)),
        "prefix_key": draw_prefix_key(jax.random.fold_in(jax.random.fold_in(key_list[13], part), 71), part),
        "prefix_value": bell_draw(part_keys[4], (PROMPTS, PROMPT, KVH * HD), 1.0, 6.0, ((1, 16),)),
        "out_weight": bell_draw(key_list[5], (QH * HD, D), (QH * HD) ** -0.5, 0.125, ((1, 16),)),
        "norm_gain": jnp.clip(1.0 + 0.1 * jax.random.normal(key_list[6], (D,), jnp.float32), 0.5, 1.5),
        "lm_head": draw_lm_head(jax.random.fold_in(key_list[13], 71), part),
        "target_ids": place_ends(skewed_wide(part_keys[8], (CONTS, CLEN), VOCAB, 2), jax.random.fold_in(part_keys[8], 3), 0, VOCAB - 1).astype(jnp.int32),
        "cont_len": place_ends(jax.random.randint(part_keys[9], (CONTS,), CLEN // 4, CLEN + 1), jax.random.fold_in(part_keys[9], 1), CLEN // 4, CLEN).astype(jnp.int32),
        "prompt_len": jax.random.randint(part_keys[10], (PROMPTS,), PROMPT // 2, PROMPT + 1).astype(jnp.int32),
        "group_of": draw_group_of(jax.random.fold_in(jax.random.fold_in(key_list[13], part), 71), part),
        "rewards": draw_rewards(jax.random.fold_in(jax.random.fold_in(key_list[13], part), 71), part),
    }


NEGATIVE = -1e+30
EPSILON = 1e-06
REWARD_FLOOR = 0.25

def normalize(hidden, norm_gain):
    widened = hidden.astype(jnp.float32)
    factor = lax.rsqrt(lax.optimization_barrier(jnp.mean(widened * widened, axis=-1, keepdims=True)) + EPSILON)
    return (widened * factor * norm_gain).astype(jnp.bfloat16)

def shard_stats(normed, token_ids, head, vocab_offset):
    logits = jnp.dot(normed, head, preferred_element_type=jnp.float32)
    maximum = lax.optimization_barrier(jnp.max(logits, axis=1))
    total_mass = lax.optimization_barrier(jnp.sum(jnp.exp(logits - maximum[:, None]), axis=1))
    columns = vocab_offset + jnp.arange(head.shape[1], dtype=jnp.int32)
    picked = lax.optimization_barrier(jnp.sum(jnp.where(token_ids[:, None] == columns[None, :], logits, 0.0), axis=1))
    return (maximum, total_mass, picked)

def join_stats(first, second):
    maximum = jnp.maximum(first[0], second[0])
    total_mass = first[1] * jnp.exp(first[0] - maximum) + second[1] * jnp.exp(second[0] - maximum)
    return (maximum, total_mass, first[2] + second[2])

def reference(cont_query, cont_key, cont_value, prefix_key, prefix_value, out_weight, norm_gain, lm_head, target_ids, cont_len, prompt_len, group_of, rewards):
    per_group = QH // KVH
    position = jnp.arange(CLEN, dtype=jnp.int32)
    causal = position[None, :] <= position[:, None]
    highest = lax.Precision.HIGHEST

    def attend(index):
        prompt = group_of[index]
        key_rows = jnp.concatenate([prefix_key[prompt], cont_key[index]], axis=0).astype(jnp.float32).reshape(PROMPT + CLEN, KVH, HD)
        value_rows = jnp.concatenate([prefix_value[prompt], cont_value[index]], axis=0).astype(jnp.float32).reshape(PROMPT + CLEN, KVH, HD)
        queries = cont_query[index].astype(jnp.float32).reshape(CLEN, KVH, per_group, HD)
        scores = jnp.einsum('tkgd,skd->tkgs', queries, key_rows, precision=highest) * HD ** (-0.5)
        early = jnp.broadcast_to((jnp.arange(PROMPT, dtype=jnp.int32) < prompt_len[prompt])[None, :], (CLEN, PROMPT))
        visible = jnp.concatenate([early, causal], axis=1)[:, None, None, :]
        scores = jnp.where(visible, scores, NEGATIVE)
        maximum = lax.optimization_barrier(jnp.max(scores, axis=-1, keepdims=True))
        weights = jnp.where(visible, jnp.exp(scores - maximum), 0.0)
        total = lax.optimization_barrier(jnp.sum(weights, axis=-1))
        mixed = jnp.einsum('tkgs,skd->tkgd', weights, value_rows, precision=highest) / total[..., None]
        return mixed.astype(jnp.bfloat16).reshape(CLEN, QH * HD)
    attended = lax.map(attend, jnp.arange(CONTS, dtype=jnp.int32)).reshape(CONTS * CLEN, QH * HD)
    hidden = jnp.dot(attended, out_weight, preferred_element_type=jnp.float32).astype(jnp.bfloat16)
    normed = normalize(hidden, norm_gain)
    token_ids = target_ids.reshape(CONTS * CLEN)
    block = VOCAB // N_SEQ

    def vocab_step(step, running):
        head = lax.dynamic_slice_in_dim(lm_head, step * block, block, 1)
        stats = shard_stats(normed, token_ids, head, step * block)
        return join_stats(running, stats)
    start_stats = (jnp.full((CONTS * CLEN,), NEGATIVE, jnp.float32), jnp.zeros((CONTS * CLEN,), jnp.float32), jnp.zeros((CONTS * CLEN,), jnp.float32))
    maximum, total_mass, picked = lax.fori_loop(0, N_SEQ, vocab_step, start_stats)
    logprob = (picked - maximum - jnp.log(total_mass)).reshape(CONTS, CLEN)
    live = position[None, :] < cont_len[:, None]
    token_logprob = jnp.where(live, logprob, 0.0)
    same_group = (group_of[:, None] == group_of[None, :]).astype(jnp.float32)
    group_mean = jnp.dot(same_group, rewards, precision=highest) / GROUP
    deviation = rewards[None, :] - group_mean[:, None]
    spread = jnp.sqrt(lax.optimization_barrier(jnp.sum(same_group * deviation * deviation, axis=1)) / (GROUP - 1))
    advantage = (rewards - group_mean) / jnp.maximum(spread, REWARD_FLOOR)
    objective = advantage * lax.optimization_barrier(jnp.sum(token_logprob, axis=1)) / cont_len.astype(jnp.float32)
    return (token_logprob, advantage, objective)
```

```python
import functools

import jax
import jax.numpy as jnp
from jax import lax
from jax.experimental import pallas as pl
from jax.experimental.pallas import tpu as pltpu
from jax.sharding import PartitionSpec as P

HD = 128
GROUP = 16
NEGATIVE = -1e30
EPSILON = 1e-06
REWARD_FLOOR = 0.25
MESH = pl.DeviceIdType.MESH
VMEM = pltpu.VMEM
LIMIT = 60 * 1024 * 1024
TILE = 1584
WPARTS = 5
SPLIT = 3
STEP = 32
WIDE = 64
PAIR = 2
QUAD = 4


def pick(table, at):
    out = table[0]
    for i in range(1, len(table)):
        out = jnp.where(at == i, table[i], out)
    return out


class Place:
    def __init__(self, n, planes):
        self.n, self.planes = n, planes
        self.lanes = n // planes
        self.half = self.lanes // 2
        self.me = lax.axis_index("seq")
        self.plane = self.me // self.lanes
        self.lane = self.me % self.lanes
        self.row = self.lane // 2
        self.core = self.lane % 2

    def device(self, plane, row, core):
        return plane * self.lanes + row * 2 + core

    def row_at(self, step):
        return (self.row + step) % self.half

    def sources(self):
        tables = []
        for p in range(self.planes):
            others = [s for s in range(self.planes) if s != p]
            others.sort(key=lambda s: (not self.passes(s, p), abs(s - p)))
            tables.append(others)
        return [
            pick([table[j] for table in tables], self.plane) for j in range(self.planes - 1)
        ]

    def ranked(self, far_first):
        tables = []
        for p in range(self.planes):
            others = [s for s in range(self.planes) if s != p]
            others.sort(key=lambda s: -abs(s - p) if far_first else abs(s - p))
            tables.append(others)
        return [
            pick([table[j] for table in tables], self.plane) for j in range(self.planes - 1)
        ]

    def passes(self, source, p):
        if source < p:
            return p + 1 < self.planes and not (source == 0 and p == 1)
        return p >= 1 and not (source == self.planes - 1 and p == self.planes - 2)


class Wire:
    def __init__(self, send_sem, recv_sem):
        self.send_sem, self.recv_sem = send_sem, recv_sem
        self.sent = []

    def send(self, src, dst, slot, target, when=None):
        copy = pltpu.make_async_remote_copy(
            src_ref=src,
            dst_ref=dst,
            send_sem=self.send_sem.at[len(self.sent)],
            recv_sem=self.recv_sem.at[slot],
            device_id={"seq": target},
            device_id_type=MESH,
        )
        self.sent.append(when)
        if when is None:
            copy.start()
        else:
            pl.when(when())(copy.start)

    def arrived(self, dst, slot, other):
        pltpu.make_async_remote_copy(
            src_ref=dst,
            dst_ref=dst,
            send_sem=self.send_sem.at[0],
            recv_sem=self.recv_sem.at[slot],
            device_id={"seq": other},
            device_id_type=MESH,
        ).wait_recv()

    def drain(self, like, other):
        for i, when in enumerate(self.sent):
            copy = pltpu.make_async_remote_copy(
                src_ref=like,
                dst_ref=like,
                send_sem=self.send_sem.at[i],
                recv_sem=self.recv_sem.at[0],
                device_id={"seq": other},
                device_id_type=MESH,
            )
            if when is None:
                copy.wait_send()
            else:
                pl.when(when())(copy.wait_send)


class Line:
    def __init__(self, at, wire, piece, slot):
        self.at, self.wire, self.piece, self.slot = at, wire, piece, slot

    def peer(self, plane):
        return self.at.device(plane, self.at.row, self.at.core)

    def send_own(self, part):
        at = self.at
        last = at.planes - 1
        mine = self.piece(part, at.plane)
        slot = self.slot(part, at.plane)
        moves = [(1, lambda: at.plane < last), (-1, lambda: at.plane > 0)]
        if at.planes > 2:
            far = jnp.where(at.plane == 0, 2, last - 2)

            def ends():
                return jnp.logical_or(at.plane == 0, at.plane == last)

            self.wire.send(mine, mine, slot, self.peer(far), ends)
        for step, when in moves:
            target = jnp.clip(at.plane + step, 0, last)
            self.wire.send(mine, mine, slot, self.peer(target), when)

    def take(self, part, source):
        at = self.at
        last = at.planes - 1
        got = self.piece(part, source)
        slot = self.slot(part, source)
        self.wire.arrived(got, slot, self.peer(source))
        def toward():
            return jnp.where(source < at.plane, at.plane + 1, at.plane - 1)

        def when():
            target = toward()
            inside = jnp.logical_and(target >= 0, target <= last)
            direct = jnp.logical_or(
                jnp.logical_and(source == 0, at.plane == 1),
                jnp.logical_and(source == last, at.plane == last - 1),
            )
            return jnp.logical_and(inside, jnp.logical_not(direct))

        self.wire.send(got, got, slot, self.peer(jnp.clip(toward(), 0, last)), when)


def layer_kernel(
    n,
    planes,
    group_ref,
    length_ref,
    length_own_ref,
    reward_ref,
    q_ref,
    ck_ref,
    cv_ref,
    pk_ref,
    pv_ref,
    ids_ref,
    w_ref,
    gain_ref,
    head_hbm,
    logprob_out,
    rating_out,
    stats_s,
    meta_s,
    meta_all,
    rating_s,
    q_s,
    ck_s,
    cv_s,
    pk_s,
    pv_s,
    att_s,
    w_s,
    hid_s,
    norm_s,
    factor_s,
    head_s,
    ids_s,
    max_s,
    sum_s,
    pick_s,
    tile_s,
    kv_send,
    kv_recv,
    q_send,
    q_recv,
    p_send,
    p_recv,
    meta_send,
    meta_recv,
    w_send,
    w_recv,
    b_send,
    b_recv,
    c_send,
    c_recv,
    stat_send,
    stat_recv,
    local_sem,
    head_sem,
):
    at = Place(n, planes)
    conts, steps, _ = q_ref.shape
    span = pk_ref.shape[1]
    width = q_ref.shape[2] // planes
    heads = width // HD
    depth = w_ref.shape[1]
    wrows = w_ref.shape[0]
    features = wrows * at.lanes
    vocab = head_hbm.shape[0]
    prompts = pk_ref.shape[0]
    block = PAIR * steps
    halves = planes // PAIR
    subs = conts * halves
    tiles, rest = vocab // TILE, vocab % TILE
    last_row = at.half - 1

    def load(tile, size):
        cut = pl.ds(pl.multiple_of(tile * TILE, 8), size)
        return pltpu.make_async_copy(head_hbm.at[cut], head_s.at[cut], head_sem.at[tile])

    for tile in range(tiles):
        load(tile, TILE).start()
    if rest:
        load(tiles, rest).start()

    lane_of = lax.broadcasted_iota(jnp.int32, (1, 128), 1)
    meta_s[...] = jnp.zeros_like(meta_s)
    for i in range(conts):
        meta_s[0:1, i * steps : (i + 1) * steps] = ids_ref[i : i + 1, :].astype(jnp.float32)
    own_rewards = jnp.zeros((1, 128), jnp.float32)
    for i in range(conts):
        own_rewards = jnp.where(lane_of == i, reward_ref[i], own_rewards)
    meta_s[1:2, :] = own_rewards

    barrier = pltpu.get_barrier_semaphore()
    for d in range(1, n):
        pl.semaphore_signal(
            barrier, inc=1, device_id={"seq": (at.me + d) % n}, device_id_type=MESH
        )
    pl.semaphore_wait(barrier, n - 1)

    locals_ = []

    def local(src, dst):
        copy = pltpu.make_async_copy(src, dst, local_sem.at[len(locals_)])
        copy.start()
        locals_.append(copy)

    sources = at.sources()
    far = at.ranked(True)
    near = at.ranked(False)

    kv = Wire(kv_send, kv_recv)

    def kv_full(part, source):
        start = pl.multiple_of(source * span, 16)
        return (pk_s, pv_s)[part // prompts].at[part % prompts, pl.ds(start, span), :]

    def kv_own(part, plane):
        cut = pl.ds(pl.multiple_of(plane * HD, 128), HD)
        return (pk_ref, pv_ref)[part // prompts].at[part % prompts, :, cut]

    def kv_share(part, source, src, core_only=False):
        slot = part * n + source
        dst = kv_full(part, source)
        if not core_only:
            for e in range(1, at.half):
                kv.send(src, dst, slot, at.device(at.plane, at.row_at(e), at.core))
        kv.send(src, dst, slot, at.device(at.plane, at.row, 1 - at.core))

    ww = Wire(w_send, w_recv)
    wpart = wrows // WPARTS

    def w_full(lane, k):
        start = pl.multiple_of(lane * wrows + k * wpart, 16)
        return w_s.at[pl.ds(start, wpart)]

    def w_core(lane, k):
        piece = w_full(lane, k)
        ww.send(piece, piece, lane * WPARTS + k, at.device(at.plane, at.row, 1 - at.core))

    def w_own(k):
        src = w_ref.at[pl.ds(k * wpart, wpart)]
        slot = at.lane * WPARTS + k
        for e in range(1, at.half):
            ww.send(src, w_full(at.lane, k), slot, at.device(at.plane, at.row_at(e), at.core))
        ww.send(src, w_full(at.lane, k), slot, at.device(at.plane, at.row, 1 - at.core))

    def w_arrived(lane, k):
        other = at.device(at.plane, at.row, 1 - at.core)
        ww.arrived(w_full(lane, k), lane * WPARTS + k, other)

    for part in range(2 * prompts):
        for target in far:
            kv.send(
                kv_own(part, target),
                kv_full(part, at.me),
                part * n + at.me,
                at.device(target, at.row, at.core),
            )
        own = kv_own(part, at.plane)
        kv_share(part, at.me, own)
        local(own, kv_full(part, at.me))
    w_own(0)
    w_own(1)

    meta = Wire(meta_send, meta_recv)
    for d in range(1, n):
        meta.send(meta_s, meta_all.at[at.me], at.me, (at.me + d) % n)
    local(meta_s, meta_all.at[at.me])

    qw = Wire(q_send, q_recv)
    pw = Wire(p_send, p_recv)

    def q_piece(i, source):
        return q_s.at[i, source]

    def c_pieces(i, source):
        return (ck_s.at[i, source], cv_s.at[i, source])

    for i in range(conts):
        for target in far:
            peer = at.device(target, at.row, at.core)
            cut = pl.ds(pl.multiple_of(target * width, 128), width)
            qw.send(q_ref.at[i, :, cut], q_piece(i, at.plane), i * planes + at.plane, peer)
            narrow = pl.ds(pl.multiple_of(target * HD, 128), HD)
            for j, ref in enumerate((ck_ref, cv_ref)):
                pw.send(
                    ref.at[i, :, narrow],
                    c_pieces(i, at.plane)[j],
                    (i * 2 + j) * planes + at.plane,
                    peer,
                )
        own = pl.ds(pl.multiple_of(at.plane * width, 128), width)
        local(q_ref.at[i, :, own], q_piece(i, at.plane))
        narrow = pl.ds(pl.multiple_of(at.plane * HD, 128), HD)
        for j, ref in enumerate((ck_ref, cv_ref)):
            local(ref.at[i, :, narrow], c_pieces(i, at.plane)[j])
    local(w_ref, w_s.at[pl.ds(pl.multiple_of(at.lane * wrows, 16), wrows)])

    max_s[...] = jnp.full_like(max_s, NEGATIVE)
    sum_s[...] = jnp.zeros_like(sum_s)
    pick_s[...] = jnp.zeros_like(pick_s)

    def kv_from_rows(plane, part):
        for e in range(1, at.half):
            source = at.device(plane, at.row_at(e), at.core)
            kv.arrived(kv_full(part, source), part * n + source, source)
            kv_share(part, source, kv_full(part, source), core_only=True)

    def kv_from_plane(plane, part):
        source = at.device(plane, at.row, at.core)
        kv.arrived(kv_full(part, source), part * n + source, source)
        kv_share(part, source, kv_full(part, source))

    for part in range(2 * prompts):
        for plane in near:
            kv_from_plane(plane, part)
        if part == prompts - 1:
            w_own(2)
        if part:
            for plane in [at.plane] + near:
                kv_from_rows(plane, part - 1)
    for k in range(3, WPARTS):
        w_own(k)
    for plane in [at.plane] + near:
        kv_from_rows(plane, 2 * prompts - 1)

    for part in range(2 * prompts):
        for plane in range(planes):
            for row in range(at.half):
                source = at.device(plane, row, 1 - at.core)
                kv.arrived(kv_full(part, source), part * n + source, source)
    for copy in locals_:
        copy.wait()

    def attend(k):
        i, h = k // halves, k % halves
        if h == 0:
            for source in sources:
                peer = at.device(source, at.row, at.core)
                qw.arrived(q_piece(i, source), i * planes + source, peer)
                for j in range(2):
                    pw.arrived(c_pieces(i, source)[j], (i * 2 + j) * planes + source, peer)

        @pl.loop(0, PAIR)
        def _(j):
            plane = h * PAIR + j
            prompt = group_ref[(plane * at.lanes + at.lane) * conts + i]
            length = length_ref[prompt]
            q = q_s[i, plane]
            rows = jnp.concatenate([q[:, h * HD : (h + 1) * HD] for h in range(heads)], axis=0)
            contract = (((1,), (1,)), ((), ()))
            early = lax.dot_general(
                rows, pk_s[prompt], contract, preferred_element_type=jnp.float32
            )
            late = lax.dot_general(
                rows, ck_s[i, plane], contract, preferred_element_type=jnp.float32
            )
            scale = HD ** (-0.5)
            column = lax.broadcasted_iota(jnp.int32, early.shape, 1)
            early = jnp.where(column < length, early * scale, NEGATIVE)
            line = lax.broadcasted_iota(jnp.int32, late.shape, 0) % steps
            late = jnp.where(
                lax.broadcasted_iota(jnp.int32, late.shape, 1) <= line, late * scale, NEGATIVE
            )
            peak = jnp.maximum(
                jnp.max(early, axis=1, keepdims=True), jnp.max(late, axis=1, keepdims=True)
            )
            early = jnp.exp(early - peak).astype(jnp.bfloat16)
            late = jnp.exp(late - peak).astype(jnp.bfloat16)
            total = jnp.sum(early.astype(jnp.float32), axis=1, keepdims=True) + jnp.sum(
                late.astype(jnp.float32), axis=1, keepdims=True
            )
            mixed = jnp.dot(early, pv_s[prompt], preferred_element_type=jnp.float32) + jnp.dot(
                late, cv_s[i, plane], preferred_element_type=jnp.float32
            )
            mixed = (mixed / total).astype(jnp.bfloat16)
            token = pl.ds(pl.multiple_of(j * steps, 16), steps)
            cut = pl.ds(pl.multiple_of(at.plane * width, 128), width)
            att_s[k, token, cut] = jnp.concatenate(
                [mixed[h * steps : (h + 1) * steps] for h in range(heads)], axis=1
            )

    bw = Wire(b_send, b_recv)

    def b_piece(i, plane):
        return att_s.at[i, :, pl.ds(pl.multiple_of(plane * width, 128), width)]

    b_line = Line(at, bw, b_piece, lambda i, plane: i * planes + plane)

    cw = Wire(c_send, c_recv)

    def c_block(i, lane, plane):
        rows = pl.ds(pl.multiple_of(lane * block, 16), block)
        cut = pl.ds(pl.multiple_of(plane * features, 128), features)
        return hid_s.at[i, rows, cut]

    def c_slot(i, lane, plane):
        return i * n + plane * at.lanes + lane

    c_line = Line(
        at,
        cw,
        lambda i, plane: c_block(i, at.lane, plane),
        lambda i, plane: c_slot(i, at.lane, plane),
    )

    def c_core(i, lane, plane):
        piece = c_block(i, lane, plane)
        cw.send(piece, piece, c_slot(i, lane, plane), at.device(at.plane, at.row, 1 - at.core))

    def c_share(i, plane):
        piece = c_block(i, at.lane, plane)
        for e in range(1, at.half):
            cw.send(
                piece,
                piece,
                c_slot(i, at.lane, plane),
                at.device(at.plane, at.row_at(e), at.core),
            )
        c_core(i, at.lane, plane)

    def c_own(i):
        c_line.send_own(i)
        c_share(i, at.plane)

    def c_take(i, plane):
        c_line.take(i, plane)
        c_share(i, plane)

    def c_rows(i, plane, e):
        lane = at.row_at(e) * 2 + at.core
        c_arrived(i, lane, plane)
        c_core(i, lane, plane)

    def c_arrived(i, lane, plane):
        cw.arrived(
            c_block(i, lane, plane),
            c_slot(i, lane, plane),
            at.device(at.plane, at.row, 1 - at.core),
        )

    def c_cores(i, row):
        for plane in range(planes):
            c_arrived(i, row * 2 + 1 - at.core, plane)

    def project(k):
        hidden = lax.dot_general(
            att_s[k], w_s[...], (((1,), (1,)), ((), ())), preferred_element_type=jnp.float32
        )
        rows = pl.ds(pl.multiple_of(at.lane * block, 16), block)
        cut = pl.ds(pl.multiple_of(at.plane * features, 128), features)
        hid_s[k, rows, cut] = hidden.astype(jnp.bfloat16)

    def normalize(k, quad):
        base = quad * QUAD * block

        @pl.loop(0, QUAD * block // WIDE)
        def _(j):
            rows = pl.ds(pl.multiple_of(base + j * WIDE, WIDE), WIDE)
            wide = hid_s[k, rows, :].astype(jnp.float32)
            square = jnp.sum(wide * wide, axis=1, keepdims=True)
            factor = lax.rsqrt(square / depth + EPSILON)
            out = pl.ds(pl.multiple_of(j * WIDE, WIDE), WIDE)
            factor_s[out] = jnp.broadcast_to(factor, (WIDE, 128))

        @pl.loop(0, QUAD * block // STEP)
        def _(j):
            rows = pl.ds(pl.multiple_of(base + j * STEP, STEP), STEP)
            out = pl.ds(pl.multiple_of(j * STEP, STEP), STEP)
            factor = factor_s[out]
            for c in range(depth // 128):
                cut = slice(c * 128, (c + 1) * 128)
                wide = hid_s[k, rows, cut].astype(jnp.float32)
                norm_s[out, cut] = (wide * factor * gain_ref[c : c + 1, :]).astype(jnp.bfloat16)

    first = [True]

    def score_group(k, quad, events, early=0):
        wait = first[0]
        first[0] = False
        tokens = QUAD * block
        start = (k * (at.lanes // QUAD) + quad) * tokens
        band = slice(start, start + tokens)

        def score(tile, size, split):
            if wait:
                load(tile, size).wait()
            part = size // split
            base = tile * TILE
            products = []
            for s in range(split):
                head = head_s[pl.ds(pl.multiple_of(base + s * part, 8), part)]
                products.append(
                    lax.dot_general(
                        head,
                        norm_s[...],
                        (((1,), (1,)), ((), ())),
                        preferred_element_type=jnp.float32,
                    )
                )
            for s, logits in enumerate(products):
                row_ = lax.broadcasted_iota(jnp.int32, logits.shape, 0)
                want = ids_s[:, band] - (base + s * part + at.me * vocab)
                chosen = jnp.where(row_ == want, logits, 0.0)
                cut = (part // 8, 8, tokens)
                before = max_s[:, band]
                best = jnp.maximum(before, jnp.max(logits.reshape(cut), axis=0))
                mass = jnp.sum(jnp.exp(logits.reshape(cut) - best[None]), axis=0)
                max_s[:, band] = best
                sum_s[:, band] = sum_s[:, band] * jnp.exp(before - best) + mass
                pick_s[:, band] += jnp.sum(chosen.reshape(cut), axis=0)

        @pl.loop(0, tiles + early)
        def _(step):
            for j, event in events:
                pl.when(step == j)(event)
            if early:
                pl.when(step >= early)(lambda: score(step - early, TILE, SPLIT))
            else:
                score(step, TILE, SPLIT)

        if rest:
            score(tiles, rest, 1)

    inner = jnp.logical_and(at.plane > 0, at.plane < planes - 1)
    outer = jnp.logical_not(inner)

    def b_relay(k):
        for source in sources:
            b_line.take(k, source)

    def b_wait(k):
        for source in sources:
            piece = b_piece(k, source)
            bw.arrived(piece, k * planes + source, at.device(source, at.row, at.core))

    def w_relay():
        for e in range(1, at.half):
            lane = at.row_at(e) * 2 + at.core
            for part in range(WPARTS):
                w_arrived(lane, part)
                w_core(lane, part)

    def w_wait():
        for row in range(at.half):
            lane = row * 2 + 1 - at.core
            for part in range(WPARTS):
                w_arrived(lane, part)

    def rows_take(k):
        for plane in [at.plane] + near:
            for e in range(1, at.half):
                c_rows(k, plane, e)

    def make_ids():
        for d in range(1, n):
            source = (at.me + d) % n
            meta.arrived(meta_all.at[source], source, source)
        for k in range(subs):
            i, h = k // halves, k % halves
            for quad in range(at.lanes // QUAD):
                got = [
                    meta_all[plane * at.lanes + lane][0:1, i * steps : (i + 1) * steps]
                    for lane in range(quad * QUAD, (quad + 1) * QUAD)
                    for plane in range(h * PAIR, (h + 1) * PAIR)
                ]
                start = (k * (at.lanes // QUAD) + quad) * QUAD * block
                ids_s[:, start : start + QUAD * block] = jnp.concatenate(got, axis=1).astype(
                    jnp.int32
                )

    def c_takes(k):
        for source in sources:
            c_take(k, source)

    def advance(k):
        project(k)
        c_own(k)

    def moment(inside, outside):
        return jnp.where(inner, inside, outside)

    assert planes == 4 and conts == 2
    peer = at.device(at.plane, at.row, 1 - at.core)

    attend(0)
    b_line.send_own(0)
    attend(1)
    b_line.send_own(1)
    attend(2)
    b_line.send_own(2)

    @pl.when(inner)
    def _():
        b_relay(0)

    attend(3)
    b_line.send_own(3)
    w_relay()

    @pl.when(inner)
    def _():
        b_relay(1)

    w_wait()

    @pl.when(outer)
    def _():
        b_wait(0)

    advance(0)

    def rate():
        shape = (n, 128)
        row_at = lax.broadcasted_iota(jnp.int32, shape, 0)
        lane_at = lax.broadcasted_iota(jnp.int32, shape, 1)
        groups = jnp.full(shape, -1, jnp.int32)
        for d in range(n):
            for i in range(conts):
                here = jnp.logical_and(row_at == d, lane_at == i)
                groups = jnp.where(here, group_ref[d * conts + i], groups)
        rewards = jnp.concatenate([meta_all[d][1:2, :] for d in range(n)], axis=0)

        def total(x):
            return jnp.sum(jnp.sum(x, axis=0, keepdims=True), axis=1, keepdims=True)

        for i in range(conts):
            same = (groups == group_ref[at.me * conts + i]).astype(jnp.float32)
            mean = total(same * rewards) / GROUP
            deviation = rewards - mean
            spread = jnp.sqrt(total(same * deviation * deviation) / (GROUP - 1))
            advantage = (reward_ref[i] - mean) / jnp.maximum(spread, REWARD_FLOOR)
            rating_s[i : i + 1, :] = jnp.broadcast_to(advantage, (1, 128))

    def settle():
        make_ids()
        kv.drain(kv_full(0, at.me), peer)
        meta.drain(meta_all.at[at.me], peer)
        qw.drain(q_piece(0, at.plane), peer)
        pw.drain(c_pieces(0, at.plane)[0], peer)
        ww.drain(w_full(at.lane, 0), peer)
        rate()

    def relays():
        b_relay(2)
        b_relay(3)

    def follow(k):
        pl.when(outer)(functools.partial(b_wait, k))
        advance(k)

    def ready(k):
        rows_take(k)
        for row in range(at.half):
            c_cores(k, row)
        normalize(k, 0)

    takes = [functools.partial(c_takes, k) for k in range(subs)]
    never = -1
    final = tiles + 2
    schedule = [
        [
            (moment(0, 1), settle),
            (moment(0, 1), takes[0]),
            (moment(1, never), relays),
            (moment(1, 0), functools.partial(follow, 1)),
            (moment(2, min(4, final)), functools.partial(follow, 2)),
            (moment(2, min(5, final)), takes[1]),
            (moment(3, min(5, final)), functools.partial(follow, 3)),
            (3, functools.partial(ready, 0)),
        ],
        [(min(1, tiles - 1), takes[2]), (min(2, tiles - 1), takes[3])],
        [(min(1, tiles - 1), functools.partial(rows_take, 3))],
        [],
    ]
    for k in range(subs):
        if k in (1, 2):
            rows_take(k)
        if k:
            for row in range(at.half):
                c_cores(k, row)
            normalize(k, 0)
        score_group(k, 0, schedule[k], 0 if k else 3)
        for quad in range(1, at.lanes // QUAD):
            normalize(k, quad)
            score_group(k, quad, [])

    tile_s[...] = jnp.zeros_like(tile_s)
    for i in range(conts):
        for lane in range(at.lanes):
            parts = [
                ((i * halves + h) * at.lanes + lane) * block for h in range(halves)
            ]

            def across(ref):
                return jnp.concatenate([ref[:, p : p + block] for p in parts], axis=1)

            peak = across(max_s)
            top = jnp.max(peak, axis=0, keepdims=True)
            mass = jnp.sum(across(sum_s) * jnp.exp(peak - top), axis=0, keepdims=True)
            tile_s[lane, i * 3 : i * 3 + 1] = top
            tile_s[lane, i * 3 + 1 : i * 3 + 2] = mass
            tile_s[lane, i * 3 + 2 : i * 3 + 3] = jnp.sum(across(pick_s), axis=0, keepdims=True)

    stat = Wire(stat_send, stat_recv)
    for d in range(1, n):
        target = (at.me + d) % n
        stat.send(tile_s.at[target % at.lanes], stats_s.at[at.me], at.me, target)
    own = pltpu.make_async_copy(tile_s.at[at.lane], stats_s.at[at.me], local_sem.at[0])
    own.start()
    bw.drain(b_piece(0, at.plane), peer)
    cw.drain(c_block(0, at.lane, at.plane), peer)
    for d in range(1, n):
        source = (at.me + d) % n
        stat.arrived(stats_s.at[source], source, source)
    own.wait()
    advantages = jnp.zeros((1, 128), jnp.float32)
    objectives = jnp.zeros((1, 128), jnp.float32)
    for i in range(conts):
        peaks = stats_s[:, i * 3, :]
        top = jnp.max(peaks, axis=0, keepdims=True)
        mass = jnp.sum(stats_s[:, i * 3 + 1, :] * jnp.exp(peaks - top), axis=0, keepdims=True)
        picked = jnp.sum(stats_s[:, i * 3 + 2, :], axis=0, keepdims=True)
        every = picked - top - jnp.log(mass)
        logprob = pick([every[:, p * steps : (p + 1) * steps] for p in range(planes)], at.plane)
        length = length_own_ref[i]
        position = lax.broadcasted_iota(jnp.int32, logprob.shape, 1)
        logprob = jnp.where(position < length, logprob, 0.0)
        logprob_out[i : i + 1, :] = logprob
        advantage = rating_s[i : i + 1, :]
        summed = jnp.sum(logprob, axis=1, keepdims=True)
        objective = advantage * summed / jnp.full((1, 128), length, jnp.int32).astype(jnp.float32)
        advantages = jnp.where(lane_of == i, advantage, advantages)
        objectives = jnp.where(lane_of == i, objective, objectives)
    rating_out[0:1, :] = advantages[:, :conts]
    rating_out[1:2, :] = objectives[:, :conts]
    stat.drain(stats_s.at[at.me], peer)


def layer(n, planes, groups, lengths, own, rewards, q, ck, cv, pk, pv, ids, w, gain, head):
    conts, steps, width = q.shape
    prompts, span, _ = pk.shape
    lanes = n // planes
    half = lanes // 2
    depth = w.shape[1]
    block = planes * steps
    total = conts * lanes * block
    sub = PAIR * steps
    subs = conts * planes // PAIR
    dma = pltpu.SemaphoreType.DMA
    vmem = pl.BlockSpec(memory_space=VMEM)
    smem = pl.BlockSpec(memory_space=pltpu.SMEM)
    bf16, f32 = jnp.bfloat16, jnp.float32
    running = VMEM((8, total), f32)
    shape = jax.ShapeDtypeStruct
    kv_sends = 2 * prompts * ((planes - 1) + half + (planes - 1) * half + planes * (half - 1))
    line_sends = 3 + planes - 1
    return pl.pallas_call(
        functools.partial(layer_kernel, n, planes),
        out_shape=(shape((conts, steps), f32), shape((2, conts), f32)),
        in_specs=[smem] * 4 + [vmem] * 8 + [pl.BlockSpec(memory_space=pl.ANY)],
        out_specs=(vmem, vmem),
        scratch_shapes=[
            VMEM((n, 8, 128), f32),
            VMEM((8, 128), f32),
            VMEM((n, 8, 128), f32),
            VMEM((conts, 128), f32),
            VMEM((conts, planes, steps, width // planes), bf16),
            VMEM((conts, planes, steps, HD), bf16),
            VMEM((conts, planes, steps, HD), bf16),
            VMEM((prompts, span * n, HD), bf16),
            VMEM((prompts, span * n, HD), bf16),
            VMEM((subs, sub, width), bf16),
            VMEM((w.shape[0] * lanes, depth), bf16),
            VMEM((subs, lanes * sub, depth), bf16),
            VMEM((QUAD * sub, depth), bf16),
            VMEM((QUAD * sub, 128), f32),
            VMEM(head.shape, bf16),
            VMEM((1, total), jnp.int32),
            running,
            running,
            running,
            VMEM((lanes, 8, 128), f32),
            dma((kv_sends,)),
            dma((2 * prompts * n,)),
            dma((conts * (planes - 1),)),
            dma((conts * planes,)),
            dma((2 * conts * (planes - 1),)),
            dma((2 * conts * planes,)),
            dma((n - 1,)),
            dma((n,)),
            dma((2 * half * WPARTS,)),
            dma((lanes * WPARTS,)),
            dma((subs * line_sends,)),
            dma((subs * planes,)),
            dma((subs * (line_sends + planes * half + planes * (half - 1)),)),
            dma((subs * n,)),
            dma((n - 1,)),
            dma((n,)),
            dma((2 * prompts + 1 + 3 * conts + 1,)),
            dma((pl.cdiv(head.shape[0], TILE),)),
        ],
        compiler_params=pltpu.CompilerParams(
            collective_id=0, has_side_effects=True, vmem_limit_bytes=LIMIT
        ),
        name="layer",
    )(groups, lengths, own, rewards, q, ck, cv, pk, pv, ids, w, gain, head)


def per_device(
    n,
    cont_query,
    cont_key,
    cont_value,
    prefix_key,
    prefix_value,
    out_weight,
    norm_gain,
    lm_head,
    target_ids,
    cont_len,
    prompt_len,
    group_of,
    rewards,
):
    token_logprob, rating = layer(
        n,
        cont_key.shape[2] // HD,
        group_of,
        prompt_len,
        cont_len,
        rewards,
        cont_query,
        cont_key,
        cont_value,
        prefix_key,
        prefix_value,
        target_ids,
        out_weight.T,
        norm_gain.reshape(-1, 128),
        lm_head.T,
    )
    return (token_logprob, rating[0], rating[1])


def solution(mesh):
    placed = (
        P(("grp", "seq"), None, None),
        P(("grp", "seq"), None, None),
        P(("grp", "seq"), None, None),
        P("grp", "seq", None),
        P("grp", "seq", None),
        P(None, "seq"),
        P(),
        P(None, "seq"),
        P(("grp", "seq"), None),
        P(("grp", "seq")),
        P("grp"),
        P("grp"),
        P(("grp", "seq")),
    )
    return jax.shard_map(
        functools.partial(per_device, mesh.shape["seq"]),
        mesh=mesh,
        in_specs=placed,
        out_specs=(P(("grp", "seq"), None), P(("grp", "seq")), P(("grp", "seq"))),
        check_vma=False,
    )
```

```python
import functools

import jax
import jax.numpy as jnp
from jax import lax
from jax.experimental import pallas as pl
from jax.experimental.pallas import tpu as pltpu
from jax.sharding import PartitionSpec as P

HD = 128
GROUP = 16
NEGATIVE = -1e30
EPSILON = 1e-06
REWARD_FLOOR = 0.25
MESH = pl.DeviceIdType.MESH
VMEM = pltpu.VMEM
LIMIT = 60 * 1024 * 1024
TILE = 1584
WPARTS = 5
SPLIT = 3
STEP = 32
WIDE = 64
PAIR = 2
QUAD = 4


def pick(table, at):
    out = table[0]
    for i in range(1, len(table)):
        out = jnp.where(at == i, table[i], out)
    return out


class Place:
    def __init__(self, n, planes):
        self.n, self.planes = n, planes
        self.lanes = n // planes
        self.half = self.lanes // 2
        self.me = lax.axis_index("seq")
        self.plane = self.me // self.lanes
        self.lane = self.me % self.lanes
        self.row = self.lane // 2
        self.core = self.lane % 2

    def device(self, plane, row, core):
        return plane * self.lanes + row * 2 + core

    def row_at(self, step):
        return (self.row + step) % self.half

    def sources(self):
        tables = []
        for p in range(self.planes):
            others = [s for s in range(self.planes) if s != p]
            others.sort(key=lambda s: (not self.passes(s, p), abs(s - p)))
            tables.append(others)
        return [
            pick([table[j] for table in tables], self.plane) for j in range(self.planes - 1)
        ]

    def ranked(self, far_first):
        tables = []
        for p in range(self.planes):
            others = [s for s in range(self.planes) if s != p]
            others.sort(key=lambda s: -abs(s - p) if far_first else abs(s - p))
            tables.append(others)
        return [
            pick([table[j] for table in tables], self.plane) for j in range(self.planes - 1)
        ]

    def passes(self, source, p):
        if source < p:
            return p + 1 < self.planes and not (source == 0 and p == 1)
        return p >= 1 and not (source == self.planes - 1 and p == self.planes - 2)


class Wire:
    def __init__(self, send_sem, recv_sem, shared=0):
        self.send_sem, self.recv_sem, self.shared = send_sem, recv_sem, shared
        self.sent = []

    def send(self, src, dst, slot, target, when=None, share=None):
        if share is None:
            share = self.shared + len(self.sent)
            self.sent.append(when)
        copy = pltpu.make_async_remote_copy(
            src_ref=src,
            dst_ref=dst,
            send_sem=self.send_sem.at[share],
            recv_sem=self.recv_sem.at[slot],
            device_id={"seq": target},
            device_id_type=MESH,
        )
        if when is None:
            copy.start()
        else:
            pl.when(when())(copy.start)

    def whole(self, ref, send, slot, other):
        return pltpu.make_async_remote_copy(
            src_ref=ref,
            dst_ref=ref,
            send_sem=self.send_sem.at[send],
            recv_sem=self.recv_sem.at[slot],
            device_id={"seq": other},
            device_id_type=MESH,
        )

    def arrived(self, dst, slot, other):
        self.whole(dst, 0, slot, other).wait_recv()

    def left(self, ref, send, other):
        self.whole(ref, send, 0, other).wait_send()

    def drain(self, like, other):
        for i, when in enumerate(self.sent):
            copy = self.whole(like, self.shared + i, 0, other)
            if when is None:
                copy.wait_send()
            else:
                pl.when(when())(copy.wait_send)


class Line:
    def __init__(self, at, wire, piece, slot):
        self.at, self.wire, self.piece, self.slot = at, wire, piece, slot

    def peer(self, plane):
        return self.at.device(plane, self.at.row, self.at.core)

    def send_own(self, part, far=True):
        at = self.at
        last = at.planes - 1
        mine = self.piece(part, at.plane)
        slot = self.slot(part, at.plane)
        moves = [(1, lambda: at.plane < last), (-1, lambda: at.plane > 0)]
        if at.planes > 2 and far:
            beyond = jnp.where(at.plane == 0, 2, last - 2)

            def ends():
                return jnp.logical_or(at.plane == 0, at.plane == last)

            self.wire.send(mine, mine, slot, self.peer(beyond), ends)
        for step, when in moves:
            target = jnp.clip(at.plane + step, 0, last)
            self.wire.send(mine, mine, slot, self.peer(target), when)

    def take(self, part, source, chain=False):
        at = self.at
        last = at.planes - 1
        got = self.piece(part, source)
        slot = self.slot(part, source)
        self.wire.arrived(got, slot, self.peer(source))
        def toward():
            return jnp.where(source < at.plane, at.plane + 1, at.plane - 1)

        def when():
            target = toward()
            inside = jnp.logical_and(target >= 0, target <= last)
            if chain:
                return inside
            direct = jnp.logical_or(
                jnp.logical_and(source == 0, at.plane == 1),
                jnp.logical_and(source == last, at.plane == last - 1),
            )
            return jnp.logical_and(inside, jnp.logical_not(direct))

        self.wire.send(got, got, slot, self.peer(jnp.clip(toward(), 0, last)), when)


def layer_kernel(
    n,
    planes,
    group_ref,
    length_ref,
    length_own_ref,
    reward_ref,
    q_ref,
    ck_ref,
    cv_ref,
    pk_ref,
    pv_ref,
    ids_ref,
    w_ref,
    gain_ref,
    head_hbm,
    result_out,
    stats_s,
    meta_s,
    meta_all,
    rating_s,
    q_s,
    ck_s,
    cv_s,
    pk_s,
    pv_s,
    att_s,
    w_s,
    hid_s,
    norm_s,
    factor_s,
    head_s,
    ids_s,
    max_s,
    sum_s,
    pick_s,
    tile_s,
    kv_send,
    kv_recv,
    q_send,
    q_recv,
    p_send,
    p_recv,
    meta_send,
    meta_recv,
    w_send,
    w_recv,
    b_send,
    b_recv,
    c_send,
    c_recv,
    stat_send,
    stat_recv,
    local_sem,
    head_sem,
):
    at = Place(n, planes)
    conts, steps, _ = q_ref.shape
    span = pk_ref.shape[1]
    width = q_ref.shape[2] // planes
    heads = width // HD
    depth = w_ref.shape[1]
    wrows = w_ref.shape[0]
    features = wrows * at.lanes
    vocab = head_hbm.shape[0]
    prompts = pk_ref.shape[0]
    block = PAIR * steps
    halves = planes // PAIR
    subs = conts * halves
    tiles, rest = vocab // TILE, vocab % TILE
    last_row = at.half - 1

    def load(tile, size):
        cut = pl.ds(pl.multiple_of(tile * TILE, 8), size)
        return pltpu.make_async_copy(head_hbm.at[cut], head_s.at[cut], head_sem.at[tile])

    for tile in range(tiles):
        load(tile, TILE).start()
    if rest:
        load(tiles, rest).start()

    lane_of = lax.broadcasted_iota(jnp.int32, (1, 128), 1)
    meta_s[...] = jnp.zeros_like(meta_s)
    for i in range(conts):
        meta_s[0:1, i * steps : (i + 1) * steps] = ids_ref[i : i + 1, :].astype(jnp.float32)
    own_rewards = jnp.zeros((1, 128), jnp.float32)
    for i in range(conts):
        own_rewards = jnp.where(lane_of == i, reward_ref[i], own_rewards)
    meta_s[1:2, :] = own_rewards

    barrier = pltpu.get_barrier_semaphore()
    for d in range(1, n):
        pl.semaphore_signal(
            barrier, inc=1, device_id={"seq": (at.me + d) % n}, device_id_type=MESH
        )
    pl.semaphore_wait(barrier, n - 1)

    locals_ = []

    def local(src, dst):
        copy = pltpu.make_async_copy(src, dst, local_sem.at[len(locals_)])
        copy.start()
        locals_.append(copy)

    sources = at.sources()
    far = at.ranked(True)
    near = at.ranked(False)

    kv = Wire(kv_send, kv_recv)

    def kv_full(part, source):
        start = pl.multiple_of(source * span, 16)
        return (pk_s, pv_s)[part].at[:, pl.ds(start, span), :]

    def kv_own(part, plane):
        cut = pl.ds(pl.multiple_of(plane * HD, 128), HD)
        return (pk_ref, pv_ref)[part].at[:, :, cut]

    kinds = planes + (at.half - 1) * planes + 1

    def z_slot(part, plane):
        return part * kinds + plane

    def row_slot(part, e, plane):
        return part * kinds + planes + (e - 1) * planes + plane

    def core_slot(part):
        return part * kinds + kinds - 1

    def kv_core(part, source, src):
        dst = kv_full(part, source)
        target = at.device(at.plane, at.row, 1 - at.core)
        kv.send(src, dst, core_slot(part), target, share=part)

    def kv_share(part, source, plane, src):
        for e in range(1, at.half):
            target = at.device(at.plane, at.row_at(e), at.core)
            slot = row_slot(part, at.half - e, plane)
            kv.send(src, kv_full(part, source), slot, target, share=part)
        kv_core(part, source, src)

    ww = Wire(w_send, w_recv, at.half - 1)
    wpart = wrows // WPARTS

    def w_full(lane):
        return w_s.at[pl.ds(pl.multiple_of(lane * wrows, 16), wrows)]

    def w_own(k):
        start = pl.multiple_of(at.lane * wrows + k * wpart, 16)
        src, dst = w_ref.at[pl.ds(k * wpart, wpart)], w_s.at[pl.ds(start, wpart)]
        for e in range(1, at.half):
            target = at.device(at.plane, at.row_at(e), at.core)
            ww.send(src, dst, at.lane, target, share=e - 1)

    def w_core(lane, src):
        other = at.device(at.plane, at.row, 1 - at.core)
        ww.send(src, w_full(lane), lane, other)

    def w_arrived(lane):
        ww.arrived(w_full(lane), lane, at.device(at.plane, at.row, 1 - at.core))

    for part in range(2):
        for target in far:
            kv.send(
                kv_own(part, target),
                kv_full(part, at.me),
                z_slot(part, at.plane),
                at.device(target, at.row, at.core),
                share=part,
            )
        own = kv_own(part, at.plane)
        kv_share(part, at.me, at.plane, own)
        local(own, kv_full(part, at.me))
    for k in range(2):
        w_own(k)

    meta = Wire(meta_send, meta_recv)
    for d in range(1, n):
        meta.send(meta_s, meta_all.at[at.me], 0, (at.me + d) % n, share=0)
    local(meta_s, meta_all.at[at.me])

    qw = Wire(q_send, q_recv)
    pw = Wire(p_send, p_recv)

    def q_piece(i, source):
        return q_s.at[i, source]

    def c_pieces(i, source):
        return (ck_s.at[i, source], cv_s.at[i, source])

    for i in range(conts):
        for target in far:
            peer = at.device(target, at.row, at.core)
            cut = pl.ds(pl.multiple_of(target * width, 128), width)
            qw.send(q_ref.at[i, :, cut], q_piece(i, at.plane), i * planes + at.plane, peer)
            narrow = pl.ds(pl.multiple_of(target * HD, 128), HD)
            for j, ref in enumerate((ck_ref, cv_ref)):
                pw.send(
                    ref.at[i, :, narrow],
                    c_pieces(i, at.plane)[j],
                    (i * 2 + j) * planes + at.plane,
                    peer,
                )
        own = pl.ds(pl.multiple_of(at.plane * width, 128), width)
        local(q_ref.at[i, :, own], q_piece(i, at.plane))
        narrow = pl.ds(pl.multiple_of(at.plane * HD, 128), HD)
        for j, ref in enumerate((ck_ref, cv_ref)):
            local(ref.at[i, :, narrow], c_pieces(i, at.plane)[j])
    local(w_ref, w_s.at[pl.ds(pl.multiple_of(at.lane * wrows, 16), wrows)])

    max_s[...] = jnp.full_like(max_s, NEGATIVE)
    sum_s[...] = jnp.zeros_like(sum_s)
    pick_s[...] = jnp.zeros_like(pick_s)

    def kv_from_rows(plane, part):
        for e in range(1, at.half):
            source = at.device(plane, at.row_at(e), at.core)
            kv.arrived(kv_full(part, source), row_slot(part, e, plane), source)
            kv_core(part, source, kv_full(part, source))

    def kv_from_plane(plane, part):
        source = at.device(plane, at.row, at.core)
        kv.arrived(kv_full(part, source), z_slot(part, plane), source)
        kv_share(part, source, plane, kv_full(part, source))

    for part in range(2):
        for plane in near:
            kv_from_plane(plane, part)
        if part:
            for plane in [at.plane] + near:
                kv_from_rows(plane, part - 1)
        else:
            w_own(2)
    for k in range(3, WPARTS):
        w_own(k)
    w_core(at.lane, w_ref)
    for plane in [at.plane] + near:
        kv_from_rows(plane, 1)

    peer = at.device(at.plane, at.row, 1 - at.core)

    def kv_many(part, count):
        return (pk_s, pv_s)[part].at[:, pl.ds(0, count * span), :]

    for part in range(2):
        kv.arrived(kv_many(part, n // 2), core_slot(part), peer)
    for copy in locals_:
        copy.wait()

    def attend(k):
        i, h = k // halves, k % halves
        if h == 0:
            for source in sources:
                peer = at.device(source, at.row, at.core)
                qw.arrived(q_piece(i, source), i * planes + source, peer)
                for j in range(2):
                    pw.arrived(c_pieces(i, source)[j], (i * 2 + j) * planes + source, peer)

        @pl.loop(0, PAIR)
        def _(j):
            plane = h * PAIR + j
            prompt = group_ref[(plane * at.lanes + at.lane) * conts + i]
            length = length_ref[prompt]
            q = q_s[i, plane]
            rows = jnp.concatenate([q[:, h * HD : (h + 1) * HD] for h in range(heads)], axis=0)
            contract = (((1,), (1,)), ((), ()))
            early = lax.dot_general(
                rows, pk_s[prompt], contract, preferred_element_type=jnp.float32
            )
            late = lax.dot_general(
                rows, ck_s[i, plane], contract, preferred_element_type=jnp.float32
            )
            scale = HD ** (-0.5)
            column = lax.broadcasted_iota(jnp.int32, early.shape, 1)
            early = jnp.where(column < length, early * scale, NEGATIVE)
            line = lax.broadcasted_iota(jnp.int32, late.shape, 0) % steps
            late = jnp.where(
                lax.broadcasted_iota(jnp.int32, late.shape, 1) <= line, late * scale, NEGATIVE
            )
            peak = jnp.maximum(
                jnp.max(early, axis=1, keepdims=True), jnp.max(late, axis=1, keepdims=True)
            )
            early = jnp.exp(early - peak).astype(jnp.bfloat16)
            late = jnp.exp(late - peak).astype(jnp.bfloat16)
            total = jnp.sum(early.astype(jnp.float32), axis=1, keepdims=True) + jnp.sum(
                late.astype(jnp.float32), axis=1, keepdims=True
            )
            mixed = jnp.dot(early, pv_s[prompt], preferred_element_type=jnp.float32) + jnp.dot(
                late, cv_s[i, plane], preferred_element_type=jnp.float32
            )
            mixed = (mixed / total).astype(jnp.bfloat16)
            token = pl.ds(pl.multiple_of(j * steps, 16), steps)
            cut = pl.ds(pl.multiple_of(at.plane * width, 128), width)
            att_s[k, token, cut] = jnp.concatenate(
                [mixed[h * steps : (h + 1) * steps] for h in range(heads)], axis=1
            )

    bw = Wire(b_send, b_recv)

    def b_piece(i, plane):
        return att_s.at[i, :, pl.ds(pl.multiple_of(plane * width, 128), width)]

    b_line = Line(at, bw, b_piece, lambda i, plane: i * planes + plane)

    cw = Wire(c_send, c_recv, subs)

    def c_block(i, lane, plane):
        rows = pl.ds(pl.multiple_of(lane * block, 16), block)
        cut = pl.ds(pl.multiple_of(plane * features, 128), features)
        return hid_s.at[i, rows, cut]

    c_line = Line(
        at,
        cw,
        lambda i, plane: c_block(i, at.lane, plane),
        z_slot,
    )

    def c_core(i, lane, plane):
        piece = c_block(i, lane, plane)
        cw.send(piece, piece, core_slot(i), peer, share=i)

    def c_share(i, plane):
        piece = c_block(i, at.lane, plane)
        for e in range(1, at.half):
            target = at.device(at.plane, at.row_at(e), at.core)
            cw.send(piece, piece, row_slot(i, at.half - e, plane), target, share=i)
        c_core(i, at.lane, plane)

    def c_own(i):
        c_line.send_own(i)
        c_share(i, at.plane)

    def c_take(i, plane):
        c_line.take(i, plane)
        c_share(i, plane)

    def c_receive(i, plane):
        cw.arrived(c_block(i, at.lane, plane), z_slot(i, plane), peer)
        c_share(i, plane)

    def c_rows(i, plane, e):
        lane = at.row_at(e) * 2 + at.core
        cw.arrived(c_block(i, lane, plane), row_slot(i, e, plane), peer)
        c_core(i, lane, plane)

    def c_many(i, count):
        return hid_s.at[i, pl.ds(0, count * block), :]

    def c_cores(i):
        cw.arrived(c_many(i, at.half), core_slot(i), peer)

    def project(k):
        hidden = lax.dot_general(
            att_s[k], w_s[...], (((1,), (1,)), ((), ())), preferred_element_type=jnp.float32
        )
        rows = pl.ds(pl.multiple_of(at.lane * block, 16), block)
        cut = pl.ds(pl.multiple_of(at.plane * features, 128), features)
        hid_s[k, rows, cut] = hidden.astype(jnp.bfloat16)

    def normalize(k, quad):
        base = quad * QUAD * block

        @pl.loop(0, QUAD * block // WIDE)
        def _(j):
            rows = pl.ds(pl.multiple_of(base + j * WIDE, WIDE), WIDE)
            wide = hid_s[k, rows, :].astype(jnp.float32)
            square = jnp.sum(wide * wide, axis=1, keepdims=True)
            factor = lax.rsqrt(square / depth + EPSILON)
            out = pl.ds(pl.multiple_of(j * WIDE, WIDE), WIDE)
            factor_s[out] = jnp.broadcast_to(factor, (WIDE, 128))

        @pl.loop(0, QUAD * block // STEP)
        def _(j):
            rows = pl.ds(pl.multiple_of(base + j * STEP, STEP), STEP)
            out = pl.ds(pl.multiple_of(j * STEP, STEP), STEP)
            factor = factor_s[out]
            for c in range(depth // 128):
                cut = slice(c * 128, (c + 1) * 128)
                wide = hid_s[k, rows, cut].astype(jnp.float32)
                norm_s[out, cut] = (wide * factor * gain_ref[c : c + 1, :]).astype(jnp.bfloat16)

    first = [True]

    def score_group(k, quad, events, early=0):
        wait = first[0]
        first[0] = False
        tokens = QUAD * block
        start = (k * (at.lanes // QUAD) + quad) * tokens
        band = slice(start, start + tokens)

        def score(tile, size, split):
            if wait:
                load(tile, size).wait()
            part = size // split
            base = tile * TILE
            products = []
            for s in range(split):
                head = head_s[pl.ds(pl.multiple_of(base + s * part, 8), part)]
                products.append(
                    lax.dot_general(
                        head,
                        norm_s[...],
                        (((1,), (1,)), ((), ())),
                        preferred_element_type=jnp.float32,
                    )
                )
            for s, logits in enumerate(products):
                row_ = lax.broadcasted_iota(jnp.int32, logits.shape, 0)
                want = ids_s[:, band] - (base + s * part + at.me * vocab)
                chosen = jnp.where(row_ == want, logits, 0.0)
                cut = (part // 8, 8, tokens)
                before = max_s[:, band]
                best = jnp.maximum(before, jnp.max(logits.reshape(cut), axis=0))
                mass = jnp.sum(jnp.exp(logits.reshape(cut) - best[None]), axis=0)
                max_s[:, band] = best
                sum_s[:, band] = sum_s[:, band] * jnp.exp(before - best) + mass
                pick_s[:, band] += jnp.sum(chosen.reshape(cut), axis=0)

        @pl.loop(0, tiles + early)
        def _(step):
            for j, event in events:
                pl.when(step == j)(event)
            if early:
                pl.when(step >= early)(lambda: score(step - early, TILE, SPLIT))
            else:
                score(step, TILE, SPLIT)

        if rest:
            score(tiles, rest, 1)

    inner = jnp.logical_and(at.plane > 0, at.plane < planes - 1)
    outer = jnp.logical_not(inner)

    def b_relay(k):
        for source in sources[:-1]:
            b_line.take(k, source)

    def b_arrived(k, source):
        piece = b_piece(k, source)
        bw.arrived(piece, k * planes + source, at.device(source, at.row, at.core))

    def b_wait(k):
        @pl.when(outer)
        def _():
            for source in sources:
                b_arrived(k, source)

        if k < 2:

            @pl.when(inner)
            def _():
                b_arrived(k, sources[-1])

    def w_relay():
        for e in range(1, at.half):
            lane = at.row_at(e) * 2 + at.core
            w_arrived(lane)
            w_core(lane, w_full(lane))

    def w_wait():
        for row in range(at.half):
            w_arrived(row * 2 + 1 - at.core)

    def rows_take(k):
        for plane in [at.plane] + near:
            for e in range(1, at.half):
                c_rows(k, plane, e)

    def make_ids():
        meta.arrived(meta_all.at[pl.ds(0, n - 1)], 0, peer)
        for k in range(subs):
            i, h = k // halves, k % halves
            for quad in range(at.lanes // QUAD):
                got = [
                    meta_all[plane * at.lanes + lane][0:1, i * steps : (i + 1) * steps]
                    for lane in range(quad * QUAD, (quad + 1) * QUAD)
                    for plane in range(h * PAIR, (h + 1) * PAIR)
                ]
                start = (k * (at.lanes // QUAD) + quad) * QUAD * block
                ids_s[:, start : start + QUAD * block] = jnp.concatenate(got, axis=1).astype(
                    jnp.int32
                )

    def c_takes(k):
        for source in sources:
            c_take(k, source)

    def advance(k):
        project(k)
        c_own(k)

    def moment(inside, outside):
        return jnp.where(inner, inside, outside)

    assert planes == 4 and conts == 2
    attend(0)
    b_line.send_own(0)
    attend(1)
    b_line.send_own(1)
    attend(2)
    b_line.send_own(2, far=False)

    @pl.when(inner)
    def _():
        b_relay(0)

    attend(3)
    b_line.send_own(3, far=False)
    w_relay()

    @pl.when(inner)
    def _():
        b_relay(1)

    w_wait()
    b_wait(0)
    advance(0)

    @pl.when(inner)
    def _():
        for k in (2, 3):
            b_line.take(k, sources[-1], chain=True)

    def rate():
        shape = (n, 128)
        row_at = lax.broadcasted_iota(jnp.int32, shape, 0)
        lane_at = lax.broadcasted_iota(jnp.int32, shape, 1)
        groups = jnp.full(shape, -1, jnp.int32)
        for d in range(n):
            for i in range(conts):
                here = jnp.logical_and(row_at == d, lane_at == i)
                groups = jnp.where(here, group_ref[d * conts + i], groups)
        rewards = jnp.concatenate([meta_all[d][1:2, :] for d in range(n)], axis=0)

        def total(x):
            return jnp.sum(jnp.sum(x, axis=0, keepdims=True), axis=1, keepdims=True)

        for i in range(conts):
            same = (groups == group_ref[at.me * conts + i]).astype(jnp.float32)
            mean = total(same * rewards) / GROUP
            deviation = rewards - mean
            spread = jnp.sqrt(total(same * deviation * deviation) / (GROUP - 1))
            advantage = (reward_ref[i] - mean) / jnp.maximum(spread, REWARD_FLOOR)
            rating_s[i : i + 1, :] = jnp.broadcast_to(advantage, (1, 128))

    def settle():
        make_ids()
        for part in range(2):
            kv.left(kv_many(part, n - 1), part, peer)
        meta.left(meta_all.at[pl.ds(0, n - 1)], 0, peer)
        qw.drain(q_piece(0, at.plane), peer)
        pw.drain(c_pieces(0, at.plane)[0], peer)
        for e in range(1, at.half):
            ww.left(w_full(at.lane), e - 1, peer)
        ww.drain(w_full(at.lane), peer)
        rate()

    def follow(k):
        b_wait(k)
        advance(k)

    def ready(k):
        rows_take(k)
        c_cores(k)
        normalize(k, 0)

    def taking(k, *which):
        def take():
            for j in which:
                c_take(k, sources[j])

        return take

    def receiving(k):
        for plane in sources:
            c_receive(k, plane)

    def sent():
        bw.drain(b_piece(0, at.plane), peer)
        cw.drain(c_block(0, at.lane, at.plane), peer)
        for k in range(subs):
            cw.left(c_many(k, at.lanes - 1), k, peer)

    def at_step(j, early=0):
        return min(j, tiles - 1) + early

    schedule = [
        [
            (moment(0, 1), settle),
            (moment(0, 1), taking(0, 0, 1, 2)),
            (moment(1, 0), functools.partial(follow, 1)),
            (moment(1, -1), functools.partial(b_relay, 2)),
            (moment(2, -1), taking(1, 0, 1, 2)),
            (moment(-1, at_step(1, 3)), functools.partial(receiving, 1)),
            (moment(2, at_step(1, 3)), functools.partial(follow, 2)),
            (moment(3, -1), functools.partial(b_relay, 3)),
            (moment(3, at_step(2, 3)), functools.partial(follow, 3)),
            (3, functools.partial(ready, 0)),
            (moment(at_step(2, 3), -1), taking(2, 0, 1, 2)),
        ],
        [
            (moment(-1, 0), functools.partial(receiving, 2)),
            (moment(0, at_step(2)), taking(3, 0, 1, 2)),
            (at_step(2), functools.partial(rows_take, 2)),
        ],
        [(at_step(2), functools.partial(rows_take, 3))],
        [(at_step(1), sent)],
    ]
    for k in range(subs):
        if k == 1:
            rows_take(k)
        if k:
            c_cores(k)
            normalize(k, 0)
        score_group(k, 0, schedule[k], 0 if k else 3)
        for quad in range(1, at.lanes // QUAD):
            normalize(k, quad)
            score_group(k, quad, [])

    tile_s[...] = jnp.zeros_like(tile_s)
    for i in range(conts):
        for lane in range(at.lanes):
            parts = [
                ((i * halves + h) * at.lanes + lane) * block for h in range(halves)
            ]

            def across(ref):
                return jnp.concatenate([ref[:, p : p + block] for p in parts], axis=1)

            peak = across(max_s)
            top = jnp.max(peak, axis=0, keepdims=True)
            mass = jnp.sum(across(sum_s) * jnp.exp(peak - top), axis=0, keepdims=True)
            tile_s[lane, i * 3 : i * 3 + 1] = top
            tile_s[lane, i * 3 + 1 : i * 3 + 2] = mass
            tile_s[lane, i * 3 + 2 : i * 3 + 3] = jnp.sum(across(pick_s), axis=0, keepdims=True)

    stat = Wire(stat_send, stat_recv)
    for d in range(1, n):
        target = (at.me + d) % n
        stat.send(tile_s.at[target % at.lanes], stats_s.at[at.me], 0, target, share=0)
    own = pltpu.make_async_copy(tile_s.at[at.lane], stats_s.at[at.me], local_sem.at[0])
    own.start()
    stat.arrived(stats_s.at[pl.ds(0, n - 1)], 0, peer)
    own.wait()
    advantages = jnp.zeros((1, 128), jnp.float32)
    objectives = jnp.zeros((1, 128), jnp.float32)
    for i in range(conts):
        peaks = stats_s[:, i * 3, :]
        top = jnp.max(peaks, axis=0, keepdims=True)
        mass = jnp.sum(stats_s[:, i * 3 + 1, :] * jnp.exp(peaks - top), axis=0, keepdims=True)
        picked = jnp.sum(stats_s[:, i * 3 + 2, :], axis=0, keepdims=True)
        every = picked - top - jnp.log(mass)
        logprob = pick([every[:, p * steps : (p + 1) * steps] for p in range(planes)], at.plane)
        length = length_own_ref[i]
        position = lax.broadcasted_iota(jnp.int32, logprob.shape, 1)
        logprob = jnp.where(position < length, logprob, 0.0)
        result_out[i : i + 1, :steps] = logprob
        advantage = rating_s[i : i + 1, :]
        summed = jnp.sum(logprob, axis=1, keepdims=True)
        objective = advantage * summed / jnp.full((1, 128), length, jnp.int32).astype(jnp.float32)
        advantages = jnp.where(lane_of == i, advantage, advantages)
        objectives = jnp.where(lane_of == i, objective, objectives)
    result_out[conts : conts + 1, :] = advantages
    result_out[conts + 1 : conts + 2, :] = objectives
    stat.left(stats_s.at[pl.ds(0, n - 1)], 0, peer)


def layer(n, planes, groups, lengths, own, rewards, q, ck, cv, pk, pv, ids, w, gain, head):
    conts, steps, width = q.shape
    prompts, span, _ = pk.shape
    lanes = n // planes
    half = lanes // 2
    depth = w.shape[1]
    block = planes * steps
    total = conts * lanes * block
    sub = PAIR * steps
    subs = conts * planes // PAIR
    dma = pltpu.SemaphoreType.DMA
    vmem = pl.BlockSpec(memory_space=VMEM)
    smem = pl.BlockSpec(memory_space=pltpu.SMEM)
    bf16, f32 = jnp.bfloat16, jnp.float32
    running = VMEM((8, total), f32)
    shape = jax.ShapeDtypeStruct
    kinds = planes + (half - 1) * planes + 1
    line_sends = 3 + planes - 1
    return pl.pallas_call(
        functools.partial(layer_kernel, n, planes),
        out_shape=shape((conts + 2, 128), f32),
        in_specs=[smem] * 4 + [vmem] * 8 + [pl.BlockSpec(memory_space=pl.ANY)],
        out_specs=vmem,
        scratch_shapes=[
            VMEM((n, 8, 128), f32),
            VMEM((8, 128), f32),
            VMEM((n, 8, 128), f32),
            VMEM((conts, 128), f32),
            VMEM((conts, planes, steps, width // planes), bf16),
            VMEM((conts, planes, steps, HD), bf16),
            VMEM((conts, planes, steps, HD), bf16),
            VMEM((prompts, span * n, HD), bf16),
            VMEM((prompts, span * n, HD), bf16),
            VMEM((subs, sub, width), bf16),
            VMEM((w.shape[0] * lanes, depth), bf16),
            VMEM((subs, lanes * sub, depth), bf16),
            VMEM((QUAD * sub, depth), bf16),
            VMEM((QUAD * sub, 128), f32),
            VMEM(head.shape, bf16),
            VMEM((1, total), jnp.int32),
            running,
            running,
            running,
            VMEM((lanes, 8, 128), f32),
            dma((2,)),
            dma((2 * kinds,)),
            dma((conts * (planes - 1),)),
            dma((conts * planes,)),
            dma((2 * conts * (planes - 1),)),
            dma((2 * conts * planes,)),
            dma((1,)),
            dma((1,)),
            dma((2 * half - 1,)),
            dma((lanes,)),
            dma((subs * line_sends,)),
            dma((subs * planes,)),
            dma((subs * (1 + line_sends),)),
            dma((subs * kinds,)),
            dma((1,)),
            dma((1,)),
            dma((2 + 1 + 3 * conts + 1,)),
            dma((pl.cdiv(head.shape[0], TILE),)),
        ],
        compiler_params=pltpu.CompilerParams(
            collective_id=0, has_side_effects=True, vmem_limit_bytes=LIMIT
        ),
        name="layer",
    )(groups, lengths, own, rewards, q, ck, cv, pk, pv, ids, w, gain, head)


def per_device(
    n,
    cont_query,
    cont_key,
    cont_value,
    prefix_key,
    prefix_value,
    out_weight,
    norm_gain,
    lm_head,
    target_ids,
    cont_len,
    prompt_len,
    group_of,
    rewards,
):
    conts, steps, _ = cont_query.shape
    result = layer(
        n,
        cont_key.shape[2] // HD,
        group_of,
        prompt_len,
        cont_len,
        rewards,
        cont_query,
        cont_key,
        cont_value,
        prefix_key,
        prefix_value,
        target_ids,
        out_weight.T,
        norm_gain.reshape(-1, 128),
        lm_head.T,
    )
    return (result[:conts, :steps], result[conts, :conts], result[conts + 1, :conts])


def solution(mesh):
    placed = (
        P(("grp", "seq"), None, None),
        P(("grp", "seq"), None, None),
        P(("grp", "seq"), None, None),
        P("grp", "seq", None),
        P("grp", "seq", None),
        P(None, "seq"),
        P(),
        P(None, "seq"),
        P(("grp", "seq"), None),
        P(("grp", "seq")),
        P("grp"),
        P("grp"),
        P(("grp", "seq")),
    )
    return jax.shard_map(
        functools.partial(per_device, mesh.shape["seq"]),
        mesh=mesh,
        in_specs=placed,
        out_specs=(P(("grp", "seq"), None), P(("grp", "seq")), P(("grp", "seq"))),
        check_vma=False,
    )
```

```python
import functools

import jax
import jax.numpy as jnp
from jax import lax
from jax.experimental import pallas as pl
from jax.experimental.pallas import tpu as pltpu
from jax.sharding import PartitionSpec as P

HD = 128
GROUP = 16
NEGATIVE = -1e30
EPSILON = 1e-06
REWARD_FLOOR = 0.25
MESH = pl.DeviceIdType.MESH
VMEM = pltpu.VMEM
LIMIT = 60 * 1024 * 1024
TILE = 1584
WPARTS = 5
SPLIT = 3
STEP = 32
WIDE = 64
PAIR = 2
QUAD = 4


def pick(table, at):
    out = table[0]
    for i in range(1, len(table)):
        out = jnp.where(at == i, table[i], out)
    return out


class Place:
    def __init__(self, n, planes):
        self.n, self.planes = n, planes
        self.lanes = n // planes
        self.half = self.lanes // 2
        self.me = lax.axis_index("seq")
        self.plane = self.me // self.lanes
        self.lane = self.me % self.lanes
        self.row = self.lane // 2
        self.core = self.lane % 2

    def device(self, plane, row, core):
        return plane * self.lanes + row * 2 + core

    def row_at(self, step):
        return (self.row + step) % self.half

    def sources(self):
        tables = []
        for p in range(self.planes):
            others = [s for s in range(self.planes) if s != p]
            others.sort(key=lambda s: (not self.passes(s, p), abs(s - p)))
            tables.append(others)
        return [
            pick([table[j] for table in tables], self.plane) for j in range(self.planes - 1)
        ]

    def ranked(self, far_first):
        tables = []
        for p in range(self.planes):
            others = [s for s in range(self.planes) if s != p]
            others.sort(key=lambda s: -abs(s - p) if far_first else abs(s - p))
            tables.append(others)
        return [
            pick([table[j] for table in tables], self.plane) for j in range(self.planes - 1)
        ]

    def passes(self, source, p):
        if source < p:
            return p + 1 < self.planes and not (source == 0 and p == 1)
        return p >= 1 and not (source == self.planes - 1 and p == self.planes - 2)


class Wire:
    def __init__(self, send_sem, recv_sem, shared=0):
        self.send_sem, self.recv_sem, self.shared = send_sem, recv_sem, shared
        self.sent = []

    def send(self, src, dst, slot, target, when=None, share=None):
        if share is None:
            share = self.shared + len(self.sent)
            self.sent.append(when)
        copy = pltpu.make_async_remote_copy(
            src_ref=src,
            dst_ref=dst,
            send_sem=self.send_sem.at[share],
            recv_sem=self.recv_sem.at[slot],
            device_id={"seq": target},
            device_id_type=MESH,
        )
        if when is None:
            copy.start()
        else:
            pl.when(when())(copy.start)

    def whole(self, ref, send, slot, other):
        return pltpu.make_async_remote_copy(
            src_ref=ref,
            dst_ref=ref,
            send_sem=self.send_sem.at[send],
            recv_sem=self.recv_sem.at[slot],
            device_id={"seq": other},
            device_id_type=MESH,
        )

    def arrived(self, dst, slot, other):
        self.whole(dst, 0, slot, other).wait_recv()

    def left(self, ref, send, other):
        self.whole(ref, send, 0, other).wait_send()

    def drain(self, like, other):
        for i, when in enumerate(self.sent):
            copy = self.whole(like, self.shared + i, 0, other)
            if when is None:
                copy.wait_send()
            else:
                pl.when(when())(copy.wait_send)


class Line:
    def __init__(self, at, wire, piece, slot):
        self.at, self.wire, self.piece, self.slot = at, wire, piece, slot

    def peer(self, plane):
        return self.at.device(plane, self.at.row, self.at.core)

    def send_own(self, part, far=True):
        at = self.at
        last = at.planes - 1
        mine = self.piece(part, at.plane)
        slot = self.slot(part, at.plane)
        moves = [(1, lambda: at.plane < last), (-1, lambda: at.plane > 0)]
        if at.planes > 2 and far:
            beyond = jnp.where(at.plane == 0, 2, last - 2)

            def ends():
                return jnp.logical_or(at.plane == 0, at.plane == last)

            self.wire.send(mine, mine, slot, self.peer(beyond), ends)
        for step, when in moves:
            target = jnp.clip(at.plane + step, 0, last)
            self.wire.send(mine, mine, slot, self.peer(target), when)

    def take(self, part, source, chain=False):
        at = self.at
        last = at.planes - 1
        got = self.piece(part, source)
        slot = self.slot(part, source)
        self.wire.arrived(got, slot, self.peer(source))
        def toward():
            return jnp.where(source < at.plane, at.plane + 1, at.plane - 1)

        def when():
            target = toward()
            inside = jnp.logical_and(target >= 0, target <= last)
            if chain:
                return inside
            direct = jnp.logical_or(
                jnp.logical_and(source == 0, at.plane == 1),
                jnp.logical_and(source == last, at.plane == last - 1),
            )
            return jnp.logical_and(inside, jnp.logical_not(direct))

        self.wire.send(got, got, slot, self.peer(jnp.clip(toward(), 0, last)), when)


def layer_kernel(
    n,
    planes,
    group_ref,
    length_ref,
    length_own_ref,
    reward_ref,
    q_ref,
    ck_ref,
    cv_ref,
    pk_ref,
    pv_ref,
    ids_ref,
    w_ref,
    gain_ref,
    head_hbm,
    result_out,
    stats_s,
    meta_s,
    meta_all,
    rating_s,
    q_s,
    ck_s,
    cv_s,
    pk_s,
    pv_s,
    att_s,
    w_s,
    hid_s,
    norm_s,
    factor_s,
    head_s,
    ids_s,
    max_s,
    sum_s,
    pick_s,
    tile_s,
    kv_send,
    kv_recv,
    q_send,
    q_recv,
    p_send,
    p_recv,
    meta_send,
    meta_recv,
    w_send,
    w_recv,
    b_send,
    b_recv,
    c_send,
    c_recv,
    stat_send,
    stat_recv,
    local_sem,
    head_sem,
):
    at = Place(n, planes)
    conts, steps, _ = q_ref.shape
    span = pk_ref.shape[1]
    width = q_ref.shape[2] // planes
    heads = width // HD
    depth = w_ref.shape[1]
    wrows = w_ref.shape[0]
    features = wrows * at.lanes
    vocab = head_hbm.shape[0]
    prompts = pk_ref.shape[0]
    block = PAIR * steps
    halves = planes // PAIR
    subs = conts * halves
    tiles, rest = vocab // TILE, vocab % TILE
    last_row = at.half - 1

    def load(tile, size):
        cut = pl.ds(pl.multiple_of(tile * TILE, 8), size)
        return pltpu.make_async_copy(head_hbm.at[cut], head_s.at[cut], head_sem.at[tile])

    for tile in range(tiles):
        load(tile, TILE).start()
    if rest:
        load(tiles, rest).start()

    lane_of = lax.broadcasted_iota(jnp.int32, (1, 128), 1)
    meta_s[...] = jnp.zeros_like(meta_s)
    for i in range(conts):
        meta_s[0:1, i * steps : (i + 1) * steps] = ids_ref[i : i + 1, :].astype(jnp.float32)
    own_rewards = jnp.zeros((1, 128), jnp.float32)
    for i in range(conts):
        own_rewards = jnp.where(lane_of == i, reward_ref[i], own_rewards)
    meta_s[1:2, :] = own_rewards

    barrier = pltpu.get_barrier_semaphore()
    for d in range(1, n):
        pl.semaphore_signal(
            barrier, inc=1, device_id={"seq": (at.me + d) % n}, device_id_type=MESH
        )
    pl.semaphore_wait(barrier, n - 1)

    locals_ = []

    def local(src, dst):
        copy = pltpu.make_async_copy(src, dst, local_sem.at[len(locals_)])
        copy.start()
        locals_.append(copy)

    sources = at.sources()
    far = at.ranked(True)
    near = at.ranked(False)

    kv = Wire(kv_send, kv_recv)

    def kv_full(part, source):
        start = pl.multiple_of(source * span, 16)
        return (pk_s, pv_s)[part].at[:, pl.ds(start, span), :]

    def kv_own(part, plane):
        cut = pl.ds(pl.multiple_of(plane * HD, 128), HD)
        return (pk_ref, pv_ref)[part].at[:, :, cut]

    kinds = planes + (at.half - 1) * planes + 1

    def z_slot(part, plane):
        return part * kinds + plane

    def row_slot(part, e, plane):
        return part * kinds + planes + (e - 1) * planes + plane

    def core_slot(part):
        return part * kinds + kinds - 1

    def kv_core(part, source, src):
        dst = kv_full(part, source)
        target = at.device(at.plane, at.row, 1 - at.core)
        kv.send(src, dst, core_slot(part), target, share=part)

    def kv_share(part, source, plane, src):
        for e in range(1, at.half):
            target = at.device(at.plane, at.row_at(e), at.core)
            slot = row_slot(part, at.half - e, plane)
            kv.send(src, kv_full(part, source), slot, target, share=part)
        kv_core(part, source, src)

    ww = Wire(w_send, w_recv, at.half - 1)
    wpart = wrows // WPARTS

    def w_full(lane):
        return w_s.at[pl.ds(pl.multiple_of(lane * wrows, 16), wrows)]

    def w_own(k):
        start = pl.multiple_of(at.lane * wrows + k * wpart, 16)
        src, dst = w_ref.at[pl.ds(k * wpart, wpart)], w_s.at[pl.ds(start, wpart)]
        for e in range(1, at.half):
            target = at.device(at.plane, at.row_at(e), at.core)
            ww.send(src, dst, at.lane, target, share=e - 1)

    def w_core(lane, src):
        other = at.device(at.plane, at.row, 1 - at.core)
        ww.send(src, w_full(lane), lane, other)

    def w_arrived(lane):
        ww.arrived(w_full(lane), lane, at.device(at.plane, at.row, 1 - at.core))

    for part in range(2):
        for target in far:
            kv.send(
                kv_own(part, target),
                kv_full(part, at.me),
                z_slot(part, at.plane),
                at.device(target, at.row, at.core),
                share=part,
            )
        own = kv_own(part, at.plane)
        kv_share(part, at.me, at.plane, own)
        local(own, kv_full(part, at.me))
    for k in range(2):
        w_own(k)

    meta = Wire(meta_send, meta_recv)
    for d in range(1, n):
        meta.send(meta_s, meta_all.at[at.me], 0, (at.me + d) % n, share=0)
    local(meta_s, meta_all.at[at.me])

    qw = Wire(q_send, q_recv)
    pw = Wire(p_send, p_recv)

    def q_piece(i, source):
        return q_s.at[i, source]

    def c_pieces(i, source):
        return (ck_s.at[i, source], cv_s.at[i, source])

    for i in range(conts):
        for target in far:
            peer = at.device(target, at.row, at.core)
            cut = pl.ds(pl.multiple_of(target * width, 128), width)
            qw.send(q_ref.at[i, :, cut], q_piece(i, at.plane), i * planes + at.plane, peer)
            narrow = pl.ds(pl.multiple_of(target * HD, 128), HD)
            for j, ref in enumerate((ck_ref, cv_ref)):
                pw.send(
                    ref.at[i, :, narrow],
                    c_pieces(i, at.plane)[j],
                    (i * 2 + j) * planes + at.plane,
                    peer,
                )
        own = pl.ds(pl.multiple_of(at.plane * width, 128), width)
        local(q_ref.at[i, :, own], q_piece(i, at.plane))
        narrow = pl.ds(pl.multiple_of(at.plane * HD, 128), HD)
        for j, ref in enumerate((ck_ref, cv_ref)):
            local(ref.at[i, :, narrow], c_pieces(i, at.plane)[j])
    local(w_ref, w_s.at[pl.ds(pl.multiple_of(at.lane * wrows, 16), wrows)])

    max_s[...] = jnp.full_like(max_s, NEGATIVE)
    sum_s[...] = jnp.zeros_like(sum_s)
    pick_s[...] = jnp.zeros_like(pick_s)

    def kv_from_rows(plane, part):
        for e in range(1, at.half):
            source = at.device(plane, at.row_at(e), at.core)
            kv.arrived(kv_full(part, source), row_slot(part, e, plane), source)
            kv_core(part, source, kv_full(part, source))

    def kv_from_plane(plane, part):
        source = at.device(plane, at.row, at.core)
        kv.arrived(kv_full(part, source), z_slot(part, plane), source)
        kv_share(part, source, plane, kv_full(part, source))

    for part in range(2):
        for plane in near:
            kv_from_plane(plane, part)
        if part:
            for plane in [at.plane] + near:
                kv_from_rows(plane, part - 1)
        else:
            w_own(2)
    for k in range(3, WPARTS):
        w_own(k)
    w_core(at.lane, w_ref)
    for plane in [at.plane] + near:
        kv_from_rows(plane, 1)

    peer = at.device(at.plane, at.row, 1 - at.core)

    def kv_many(part, count):
        return (pk_s, pv_s)[part].at[:, pl.ds(0, count * span), :]

    for part in range(2):
        kv.arrived(kv_many(part, n // 2), core_slot(part), peer)
    for copy in locals_:
        copy.wait()

    def attend(k):
        i, h = k // halves, k % halves
        if h == 0:
            for source in sources:
                peer = at.device(source, at.row, at.core)
                qw.arrived(q_piece(i, source), i * planes + source, peer)
                for j in range(2):
                    pw.arrived(c_pieces(i, source)[j], (i * 2 + j) * planes + source, peer)

        @pl.loop(0, PAIR)
        def _(j):
            plane = h * PAIR + j
            prompt = group_ref[(plane * at.lanes + at.lane) * conts + i]
            length = length_ref[prompt]
            q = q_s[i, plane]
            rows = jnp.concatenate([q[:, h * HD : (h + 1) * HD] for h in range(heads)], axis=0)
            contract = (((1,), (1,)), ((), ()))
            early = lax.dot_general(
                rows, pk_s[prompt], contract, preferred_element_type=jnp.float32
            )
            late = lax.dot_general(
                rows, ck_s[i, plane], contract, preferred_element_type=jnp.float32
            )
            scale = HD ** (-0.5)
            column = lax.broadcasted_iota(jnp.int32, early.shape, 1)
            early = jnp.where(column < length, early * scale, NEGATIVE)
            line = lax.broadcasted_iota(jnp.int32, late.shape, 0) % steps
            late = jnp.where(
                lax.broadcasted_iota(jnp.int32, late.shape, 1) <= line, late * scale, NEGATIVE
            )
            peak = jnp.maximum(
                jnp.max(early, axis=1, keepdims=True), jnp.max(late, axis=1, keepdims=True)
            )
            early = jnp.exp(early - peak).astype(jnp.bfloat16)
            late = jnp.exp(late - peak).astype(jnp.bfloat16)
            total = jnp.sum(early.astype(jnp.float32), axis=1, keepdims=True) + jnp.sum(
                late.astype(jnp.float32), axis=1, keepdims=True
            )
            mixed = jnp.dot(early, pv_s[prompt], preferred_element_type=jnp.float32) + jnp.dot(
                late, cv_s[i, plane], preferred_element_type=jnp.float32
            )
            mixed = (mixed / total).astype(jnp.bfloat16)
            token = pl.ds(pl.multiple_of(j * steps, 16), steps)
            cut = pl.ds(pl.multiple_of(at.plane * width, 128), width)
            att_s[k, token, cut] = jnp.concatenate(
                [mixed[h * steps : (h + 1) * steps] for h in range(heads)], axis=1
            )

    bw = Wire(b_send, b_recv)

    def b_piece(i, plane):
        return att_s.at[i, :, pl.ds(pl.multiple_of(plane * width, 128), width)]

    b_line = Line(at, bw, b_piece, lambda i, plane: i * planes + plane)

    cw = Wire(c_send, c_recv, subs)

    def c_block(i, lane, plane):
        rows = pl.ds(pl.multiple_of(lane * block, 16), block)
        cut = pl.ds(pl.multiple_of(plane * features, 128), features)
        return hid_s.at[i, rows, cut]

    c_line = Line(
        at,
        cw,
        lambda i, plane: c_block(i, at.lane, plane),
        z_slot,
    )

    def c_core(i, lane, plane):
        piece = c_block(i, lane, plane)
        cw.send(piece, piece, core_slot(i), peer, share=i)

    def c_share(i, plane):
        piece = c_block(i, at.lane, plane)
        for e in range(1, at.half):
            target = at.device(at.plane, at.row_at(e), at.core)
            cw.send(piece, piece, row_slot(i, at.half - e, plane), target, share=i)
        c_core(i, at.lane, plane)

    def c_own(i):
        c_line.send_own(i)
        c_share(i, at.plane)

    def c_take(i, plane):
        c_line.take(i, plane)
        c_share(i, plane)

    def c_receive(i, plane):
        cw.arrived(c_block(i, at.lane, plane), z_slot(i, plane), peer)
        c_share(i, plane)

    def c_rows(i, plane, e):
        lane = at.row_at(e) * 2 + at.core
        cw.arrived(c_block(i, lane, plane), row_slot(i, e, plane), peer)
        c_core(i, lane, plane)

    def c_many(i, count):
        return hid_s.at[i, pl.ds(0, count * block), :]

    def c_cores(i):
        cw.arrived(c_many(i, at.half), core_slot(i), peer)

    def project(k):
        hidden = lax.dot_general(
            att_s[k], w_s[...], (((1,), (1,)), ((), ())), preferred_element_type=jnp.float32
        )
        rows = pl.ds(pl.multiple_of(at.lane * block, 16), block)
        cut = pl.ds(pl.multiple_of(at.plane * features, 128), features)
        hid_s[k, rows, cut] = hidden.astype(jnp.bfloat16)

    def normalize(k, quad):
        base = quad * QUAD * block

        @pl.loop(0, QUAD * block // WIDE)
        def _(j):
            rows = pl.ds(pl.multiple_of(base + j * WIDE, WIDE), WIDE)
            wide = hid_s[k, rows, :].astype(jnp.float32)
            square = jnp.sum(wide * wide, axis=1, keepdims=True)
            factor = lax.rsqrt(square / depth + EPSILON)
            out = pl.ds(pl.multiple_of(j * WIDE, WIDE), WIDE)
            factor_s[out] = jnp.broadcast_to(factor, (WIDE, 128))

        @pl.loop(0, QUAD * block // STEP)
        def _(j):
            rows = pl.ds(pl.multiple_of(base + j * STEP, STEP), STEP)
            out = pl.ds(pl.multiple_of(j * STEP, STEP), STEP)
            factor = factor_s[out]
            for c in range(depth // 128):
                cut = slice(c * 128, (c + 1) * 128)
                wide = hid_s[k, rows, cut].astype(jnp.float32)
                norm_s[out, cut] = (wide * factor * gain_ref[c : c + 1, :]).astype(jnp.bfloat16)

    first = [True]

    def score_group(k, quad, events, early=0):
        wait = first[0]
        first[0] = False
        tokens = QUAD * block
        start = (k * (at.lanes // QUAD) + quad) * tokens
        band = slice(start, start + tokens)

        def score(tile, size, split):
            if wait:
                load(tile, size).wait()
            part = size // split
            base = tile * TILE
            products = []
            for s in range(split):
                head = head_s[pl.ds(pl.multiple_of(base + s * part, 8), part)]
                products.append(
                    lax.dot_general(
                        head,
                        norm_s[...],
                        (((1,), (1,)), ((), ())),
                        preferred_element_type=jnp.float32,
                    )
                )
            for s, logits in enumerate(products):
                row_ = lax.broadcasted_iota(jnp.int32, logits.shape, 0)
                want = ids_s[:, band] - (base + s * part + at.me * vocab)
                chosen = jnp.where(row_ == want, logits, 0.0)
                cut = (part // 8, 8, tokens)
                before = max_s[:, band]
                best = jnp.maximum(before, jnp.max(logits.reshape(cut), axis=0))
                mass = jnp.sum(jnp.exp(logits.reshape(cut) - best[None]), axis=0)
                max_s[:, band] = best
                sum_s[:, band] = sum_s[:, band] * jnp.exp(before - best) + mass
                pick_s[:, band] += jnp.sum(chosen.reshape(cut), axis=0)

        @pl.loop(0, tiles + early)
        def _(step):
            for j, event in events:
                pl.when(step == j)(event)
            if early:
                pl.when(step >= early)(lambda: score(step - early, TILE, SPLIT))
            else:
                score(step, TILE, SPLIT)

        if rest:
            score(tiles, rest, 1)

    inner = jnp.logical_and(at.plane > 0, at.plane < planes - 1)
    outer = jnp.logical_not(inner)

    def b_relay(k):
        for source in sources[:-1]:
            b_line.take(k, source)

    def b_arrived(k, source):
        piece = b_piece(k, source)
        bw.arrived(piece, k * planes + source, at.device(source, at.row, at.core))

    def b_wait(k):
        @pl.when(outer)
        def _():
            for source in sources:
                b_arrived(k, source)

        if k < 2:

            @pl.when(inner)
            def _():
                b_arrived(k, sources[-1])

    def w_relay():
        for e in range(1, at.half):
            lane = at.row_at(e) * 2 + at.core
            w_arrived(lane)
            w_core(lane, w_full(lane))

    def w_wait():
        for row in range(at.half):
            w_arrived(row * 2 + 1 - at.core)

    def rows_take(k):
        for plane in [at.plane] + near:
            for e in range(1, at.half):
                c_rows(k, plane, e)

    def make_ids():
        meta.arrived(meta_all.at[pl.ds(0, n - 1)], 0, peer)
        for k in range(subs):
            i, h = k // halves, k % halves
            for quad in range(at.lanes // QUAD):
                got = [
                    meta_all[plane * at.lanes + lane][0:1, i * steps : (i + 1) * steps]
                    for lane in range(quad * QUAD, (quad + 1) * QUAD)
                    for plane in range(h * PAIR, (h + 1) * PAIR)
                ]
                start = (k * (at.lanes // QUAD) + quad) * QUAD * block
                ids_s[:, start : start + QUAD * block] = jnp.concatenate(got, axis=1).astype(
                    jnp.int32
                )

    def c_takes(k):
        for source in sources:
            c_take(k, source)

    def advance(k):
        project(k)
        c_own(k)

    def moment(inside, outside):
        return jnp.where(inner, inside, outside)

    assert planes == 4 and conts == 2
    attend(0)
    b_line.send_own(0)
    attend(1)
    b_line.send_own(1)
    attend(2)
    b_line.send_own(2, far=False)

    @pl.when(inner)
    def _():
        b_relay(0)

    attend(3)
    b_line.send_own(3, far=False)
    w_relay()

    @pl.when(inner)
    def _():
        b_relay(1)

    w_wait()
    b_wait(0)
    advance(0)

    @pl.when(inner)
    def _():
        for k in (2, 3):
            b_line.take(k, sources[-1], chain=True)

    def rate():
        shape = (n, 128)
        row_at = lax.broadcasted_iota(jnp.int32, shape, 0)
        lane_at = lax.broadcasted_iota(jnp.int32, shape, 1)
        groups = jnp.full(shape, -1, jnp.int32)
        for d in range(n):
            for i in range(conts):
                here = jnp.logical_and(row_at == d, lane_at == i)
                groups = jnp.where(here, group_ref[d * conts + i], groups)
        rewards = jnp.concatenate([meta_all[d][1:2, :] for d in range(n)], axis=0)

        def total(x):
            return jnp.sum(jnp.sum(x, axis=0, keepdims=True), axis=1, keepdims=True)

        for i in range(conts):
            same = (groups == group_ref[at.me * conts + i]).astype(jnp.float32)
            mean = total(same * rewards) / GROUP
            deviation = rewards - mean
            spread = jnp.sqrt(total(same * deviation * deviation) / (GROUP - 1))
            advantage = (reward_ref[i] - mean) / jnp.maximum(spread, REWARD_FLOOR)
            rating_s[i : i + 1, :] = jnp.broadcast_to(advantage, (1, 128))

    def settle():
        make_ids()
        for part in range(2):
            kv.left(kv_many(part, n - 1), part, peer)
        meta.left(meta_all.at[pl.ds(0, n - 1)], 0, peer)
        qw.drain(q_piece(0, at.plane), peer)
        pw.drain(c_pieces(0, at.plane)[0], peer)
        for e in range(1, at.half):
            ww.left(w_full(at.lane), e - 1, peer)
        ww.drain(w_full(at.lane), peer)
        rate()

    def follow(k):
        b_wait(k)
        advance(k)

    def ready(k):
        rows_take(k)
        c_cores(k)
        normalize(k, 0)

    def taking(k, *which):
        def take():
            for j in which:
                c_take(k, sources[j])

        return take

    def receiving(k):
        for plane in sources:
            c_receive(k, plane)

    def sent():
        bw.drain(b_piece(0, at.plane), peer)
        cw.drain(c_block(0, at.lane, at.plane), peer)
        for k in range(subs):
            cw.left(c_many(k, at.lanes - 1), k, peer)

    def at_step(j, early=0):
        return min(j, tiles - 1) + early

    schedule = [
        [
            (moment(0, 1), settle),
            (moment(0, 1), taking(0, 0, 1, 2)),
            (moment(1, 0), functools.partial(follow, 1)),
            (moment(1, -1), functools.partial(b_relay, 2)),
            (moment(2, -1), taking(1, 0, 1, 2)),
            (moment(-1, at_step(1, 3)), functools.partial(receiving, 1)),
            (moment(2, at_step(1, 3)), functools.partial(follow, 2)),
            (moment(3, -1), functools.partial(b_relay, 3)),
            (moment(3, at_step(2, 3)), functools.partial(follow, 3)),
            (3, functools.partial(ready, 0)),
            (moment(at_step(2, 3), -1), taking(2, 0, 1, 2)),
        ],
        [
            (moment(-1, 0), functools.partial(receiving, 2)),
            (moment(0, at_step(2)), taking(3, 0, 1, 2)),
            (at_step(2), functools.partial(rows_take, 2)),
        ],
        [(at_step(2), functools.partial(rows_take, 3))],
        [(at_step(1), sent)],
    ]
    for k in range(subs):
        if k == 1:
            rows_take(k)
        if k:
            c_cores(k)
            normalize(k, 0)
        score_group(k, 0, schedule[k], 0 if k else 3)
        for quad in range(1, at.lanes // QUAD):
            normalize(k, quad)
            score_group(k, quad, [])

    tile_s[...] = jnp.zeros_like(tile_s)
    for i in range(conts):
        for lane in range(at.lanes):
            parts = [
                ((i * halves + h) * at.lanes + lane) * block for h in range(halves)
            ]

            def across(ref):
                return jnp.concatenate([ref[:, p : p + block] for p in parts], axis=1)

            peak = across(max_s)
            top = jnp.max(peak, axis=0, keepdims=True)
            mass = jnp.sum(across(sum_s) * jnp.exp(peak - top), axis=0, keepdims=True)
            tile_s[lane, i * 3 : i * 3 + 1] = top
            tile_s[lane, i * 3 + 1 : i * 3 + 2] = mass
            tile_s[lane, i * 3 + 2 : i * 3 + 3] = jnp.sum(across(pick_s), axis=0, keepdims=True)

    stat = Wire(stat_send, stat_recv)
    for d in range(1, n):
        target = (at.me + d) % n
        stat.send(tile_s.at[target % at.lanes], stats_s.at[at.me], 0, target, share=0)
    own = pltpu.make_async_copy(tile_s.at[at.lane], stats_s.at[at.me], local_sem.at[0])
    own.start()
    stat.arrived(stats_s.at[pl.ds(0, n - 1)], 0, peer)
    own.wait()
    advantages = jnp.zeros((1, 128), jnp.float32)
    objectives = jnp.zeros((1, 128), jnp.float32)
    for i in range(conts):
        peaks = stats_s[:, i * 3, :]
        top = jnp.max(peaks, axis=0, keepdims=True)
        mass = jnp.sum(stats_s[:, i * 3 + 1, :] * jnp.exp(peaks - top), axis=0, keepdims=True)
        picked = jnp.sum(stats_s[:, i * 3 + 2, :], axis=0, keepdims=True)
        every = picked - top - jnp.log(mass)
        logprob = pick([every[:, p * steps : (p + 1) * steps] for p in range(planes)], at.plane)
        length = length_own_ref[i]
        position = lax.broadcasted_iota(jnp.int32, logprob.shape, 1)
        logprob = jnp.where(position < length, logprob, 0.0)
        result_out[i : i + 1, :steps] = logprob
        advantage = rating_s[i : i + 1, :]
        summed = jnp.sum(logprob, axis=1, keepdims=True)
        objective = advantage * summed / jnp.full((1, 128), length, jnp.int32).astype(jnp.float32)
        advantages = jnp.where(lane_of == i, advantage, advantages)
        objectives = jnp.where(lane_of == i, objective, objectives)
    result_out[conts : conts + 1, :] = advantages
    result_out[conts + 1 : conts + 2, :] = objectives
    stat.left(stats_s.at[pl.ds(0, n - 1)], 0, peer)


def layer(n, planes, groups, lengths, own, rewards, q, ck, cv, pk, pv, ids, w, gain, head):
    conts, steps, width = q.shape
    prompts, span, _ = pk.shape
    lanes = n // planes
    half = lanes // 2
    depth = w.shape[1]
    block = planes * steps
    total = conts * lanes * block
    sub = PAIR * steps
    subs = conts * planes // PAIR
    dma = pltpu.SemaphoreType.DMA
    vmem = pl.BlockSpec(memory_space=VMEM)
    smem = pl.BlockSpec(memory_space=pltpu.SMEM)
    bf16, f32 = jnp.bfloat16, jnp.float32
    running = VMEM((8, total), f32)
    shape = jax.ShapeDtypeStruct
    kinds = planes + (half - 1) * planes + 1
    line_sends = 3 + planes - 1
    return pl.pallas_call(
        functools.partial(layer_kernel, n, planes),
        out_shape=shape((conts + 2, 128), f32),
        in_specs=[smem] * 4 + [vmem] * 8 + [pl.BlockSpec(memory_space=pl.ANY)],
        out_specs=vmem,
        scratch_shapes=[
            VMEM((n, 8, 128), f32),
            VMEM((8, 128), f32),
            VMEM((n, 8, 128), f32),
            VMEM((conts, 128), f32),
            VMEM((conts, planes, steps, width // planes), bf16),
            VMEM((conts, planes, steps, HD), bf16),
            VMEM((conts, planes, steps, HD), bf16),
            VMEM((prompts, span * n, HD), bf16),
            VMEM((prompts, span * n, HD), bf16),
            VMEM((subs, sub, width), bf16),
            VMEM((w.shape[0] * lanes, depth), bf16),
            VMEM((subs, lanes * sub, depth), bf16),
            VMEM((QUAD * sub, depth), bf16),
            VMEM((QUAD * sub, 128), f32),
            VMEM(head.shape, bf16),
            VMEM((1, total), jnp.int32),
            running,
            running,
            running,
            VMEM((lanes, 8, 128), f32),
            dma((2,)),
            dma((2 * kinds,)),
            dma((conts * (planes - 1),)),
            dma((conts * planes,)),
            dma((2 * conts * (planes - 1),)),
            dma((2 * conts * planes,)),
            dma((1,)),
            dma((1,)),
            dma((2 * half - 1,)),
            dma((lanes,)),
            dma((subs * line_sends,)),
            dma((subs * planes,)),
            dma((subs * (1 + line_sends),)),
            dma((subs * kinds,)),
            dma((1,)),
            dma((1,)),
            dma((2 + 1 + 3 * conts + 1,)),
            dma((pl.cdiv(head.shape[0], TILE),)),
        ],
        compiler_params=pltpu.CompilerParams(
            collective_id=0, has_side_effects=True, vmem_limit_bytes=LIMIT
        ),
        name="layer",
    )(groups, lengths, own, rewards, q, ck, cv, pk, pv, ids, w, gain, head)


def finish_kernel(result_ref, logprob_ref, advantage_ref, objective_ref):
    conts, steps = logprob_ref.shape
    logprob_ref[...] = result_ref[:conts, :steps]
    advantage_ref[...] = result_ref[conts : conts + 1, :conts]
    objective_ref[...] = result_ref[conts + 1 : conts + 2, :conts]


def finish(conts, steps, result):
    vmem = pl.BlockSpec(memory_space=VMEM)
    shape = jax.ShapeDtypeStruct
    return pl.pallas_call(
        finish_kernel,
        out_shape=(
            shape((conts, steps), jnp.float32),
            shape((1, conts), jnp.float32),
            shape((1, conts), jnp.float32),
        ),
        in_specs=[vmem],
        out_specs=(vmem, vmem, vmem),
        name="finish",
    )(result)


def per_device(
    n,
    cont_query,
    cont_key,
    cont_value,
    prefix_key,
    prefix_value,
    out_weight,
    norm_gain,
    lm_head,
    target_ids,
    cont_len,
    prompt_len,
    group_of,
    rewards,
):
    conts, steps, _ = cont_query.shape
    result = layer(
        n,
        cont_key.shape[2] // HD,
        group_of,
        prompt_len,
        cont_len,
        rewards,
        cont_query,
        cont_key,
        cont_value,
        prefix_key,
        prefix_value,
        target_ids,
        out_weight.T,
        norm_gain.reshape(-1, 128),
        lm_head.T,
    )
    logprob, advantage, objective = finish(conts, steps, result)
    return (logprob, advantage.reshape(conts), objective.reshape(conts))


def solution(mesh):
    placed = (
        P(("grp", "seq"), None, None),
        P(("grp", "seq"), None, None),
        P(("grp", "seq"), None, None),
        P("grp", "seq", None),
        P("grp", "seq", None),
        P(None, "seq"),
        P(),
        P(None, "seq"),
        P(("grp", "seq"), None),
        P(("grp", "seq")),
        P("grp"),
        P("grp"),
        P(("grp", "seq")),
    )
    return jax.shard_map(
        functools.partial(per_device, mesh.shape["seq"]),
        mesh=mesh,
        in_specs=placed,
        out_specs=(P(("grp", "seq"), None), P(("grp", "seq")), P(("grp", "seq"))),
        check_vma=False,
    )
```
